16 devices in a mesh: rep: 1, dp: 16 (over x, y, z, core).
Axes of the slice: x: 2, y: 2, z: 2, core: 2. Of those that a mesh axis runs over, the one named last changes fastest.
Arguments:
- x: bfloat16 [16, 2048, 768], P(('rep', 'dp'))
- dy: bfloat16 [16, 2048, 768], P(('rep', 'dp'))
- wq: bfloat16 [2, 768, 768], replicated
- wk: bfloat16 [2, 768, 256], replicated
- wv: bfloat16 [2, 768, 256], replicated
- wo: bfloat16 [2, 768, 768], replicated
- w_gate: bfloat16 [2, 768, 2304], replicated
- w_up: bfloat16 [2, 768, 2304], replicated
- w_down: bfloat16 [2, 2304, 768], replicated
- m_wq: float32 [2, 768, 768], replicated
- m_wk: float32 [2, 768, 256], replicated
- m_wv: float32 [2, 768, 256], replicated
- m_wo: float32 [2, 768, 768], replicated
- m_w_gate: float32 [2, 768, 2304], replicated
- m_w_up: float32 [2, 768, 2304], replicated
- m_w_down: float32 [2, 2304, 768], replicated
- v_wq: float32 [2, 768, 768], replicated
- v_wk: float32 [2, 768, 256], replicated
- v_wv: float32 [2, 768, 256], replicated
- v_wo: float32 [2, 768, 768], replicated
- v_w_gate: float32 [2, 768, 2304], replicated
- v_w_up: float32 [2, 768, 2304], replicated
- v_w_down: float32 [2, 2304, 768], replicated
Outputs:
- output 1: bfloat16 [2, 768, 768], P('rep')
- output 2: bfloat16 [2, 768, 256], P('rep')
- output 3: bfloat16 [2, 768, 256], P('rep')
- output 4: bfloat16 [2, 768, 768], P('rep')
- output 5: bfloat16 [2, 768, 2304], P('rep')
- output 6: bfloat16 [2, 768, 2304], P('rep')
- output 7: bfloat16 [2, 2304, 768], P('rep')
- output 8: float32 [2, 768, 768], P('rep')
- output 9: float32 [2, 768, 256], P('rep')
- output 10: float32 [2, 768, 256], P('rep')
- output 11: float32 [2, 768, 768], P('rep')
- output 12: float32 [2, 768, 2304], P('rep')
- output 13: float32 [2, 768, 2304], P('rep')
- output 14: float32 [2, 2304, 768], P('rep')
- output 15: float32 [2, 768, 768], P('rep')
- output 16: float32 [2, 768, 256], P('rep')
- output 17: float32 [2, 768, 256], P('rep')
- output 18: float32 [2, 768, 768], P('rep')
- output 19: float32 [2, 768, 2304], P('rep')
- output 20: float32 [2, 768, 2304], P('rep')
- output 21: float32 [2, 2304, 768], P('rep')
All inputs are finite; a program needn't handle non-finite values.
Results may differ from the reference program's by a relative error of at most 0.0262.
Values are sent between devices in bfloat16 or wider.
A program may use at most 2.5 GiB of HBM per device.

```python
import jax
import jax.numpy as jnp
from jax import lax

SEQUENCES = 16
TOKENS = 2048
D = 768
HEADS = 6
KV_HEADS = 2
HEAD = 128
FF = 2304
LAYERS = 2
THETA = 10000
NAMES = ("wq", "wk", "wv", "wo", "w_gate", "w_up", "w_down")
SHAPES = {
    "wq": (LAYERS, D, HEADS * HEAD),
    "wk": (LAYERS, D, KV_HEADS * HEAD),
    "wv": (LAYERS, D, KV_HEADS * HEAD),
    "wo": (LAYERS, HEADS * HEAD, D),
    "w_gate": (LAYERS, D, FF),
    "w_up": (LAYERS, D, FF),
    "w_down": (LAYERS, FF, D),
}


def bump(key, n, height):
    away = (jnp.arange(n, dtype=jnp.int32) - jax.random.randint(key, (), 0, n, jnp.int32)) % n
    return jnp.where(away < n // 8, height, 1.0)


def together(key, own, strength):
    shared = jax.random.normal(key, own.shape[1:], jnp.float32)
    return (own + strength * shared) * lax.rsqrt(1 + strength * strength)


def setup_inputs(seed: int = 0, part: int = 0) -> dict:
    kx, kdy, ka, kb, kz, kf, kh, kl, *keys = jax.random.split(jax.random.key(seed), 8 + 3 * len(NAMES))
    kx, kdy, ka, kb = (jax.random.fold_in(k, part) for k in (kx, kdy, ka, kb))
    kw, km, kv = (keys[i::3] for i in range(3))
    shape = (SEQUENCES, TOKENS, D)
    much_x, much_dy = jax.random.uniform(kz, (2,), jnp.float32, 0.0, 1.0)
    loud = 2.0 ** jax.random.uniform(jax.random.fold_in(kz, 1), (), jnp.float32, -1.0, 2.0)
    layers = 2.0 ** jax.random.uniform(kl, (LAYERS, 1, 1), jnp.float32, -1.0, 1.0)
    times = {"wq": 1.0, "wk": 1.0, "wv": 2.0, "wo": layers, "w_gate": 1.0, "w_up": bump(kh, FF, 4.0), "w_down": layers}
    x = together(ka, jax.random.normal(kx, shape, jnp.float32), much_x) * bump(kf, D, 4.0)
    dy = together(kb, jax.random.normal(kdy, shape, jnp.float32), much_dy)
    drawn = {"x": x.astype(jnp.bfloat16), "dy": (loud * dy * (SEQUENCES * TOKENS) ** -0.5).astype(jnp.bfloat16)}
    for key, name in zip(kw, NAMES, strict=True):
        drawn[name] = (jax.random.normal(key, SHAPES[name], jnp.float32) * SHAPES[name][1] ** -0.5 * times[name]).astype(jnp.bfloat16)
    for key, name in zip(km, NAMES, strict=True):
        drawn[f"m_{name}"] = 0.1 * jax.random.normal(key, SHAPES[name], jnp.float32)
    for key, name in zip(kv, NAMES, strict=True):
        drawn[f"v_{name}"] = jax.random.uniform(key, SHAPES[name], jnp.float32, 0.02, 0.06)
    return drawn


def matmul(a, w):
    return jnp.dot(a, w, preferred_element_type=jnp.float32).astype(jnp.bfloat16)


def normed(h):
    wide = h.astype(jnp.float32)
    scale = lax.rsqrt(jnp.mean(wide**2, -1, keepdims=True) + 1e-6)
    return (wide * scale).astype(jnp.bfloat16)


def turned(t, theta):
    half = t.shape[-1] // 2
    angle = jnp.arange(t.shape[0], dtype=jnp.float32)[:, None] * theta ** (-jnp.arange(half, dtype=jnp.float32) / half)
    cos, sin = jnp.cos(angle)[:, None], jnp.sin(angle)[:, None]
    a, b = t[..., :half].astype(jnp.float32), t[..., half:].astype(jnp.float32)
    return jnp.concatenate([a * cos - b * sin, b * cos + a * sin], -1).astype(jnp.bfloat16)


def seen_by(q, k, v):
    tokens, kv = q.shape[0], k.shape[1]
    q = q.reshape(tokens, kv, -1, q.shape[-1])
    scores = jnp.einsum("tgsd,ugd->gstu", q.astype(jnp.float32), k.astype(jnp.float32)) * q.shape[-1] ** -0.5
    place = jnp.arange(tokens)
    weights = jax.nn.softmax(jnp.where(place[:, None] >= place, scores, -jnp.inf), -1).astype(jnp.bfloat16)
    return jnp.einsum("gstu,ugd->tgsd", weights.astype(jnp.float32), v.astype(jnp.float32)).astype(jnp.bfloat16).reshape(tokens, -1)


def layer(h, w):
    a = normed(h)
    q, k = (turned(matmul(a, w[name]).reshape(h.shape[0], -1, HEAD), THETA) for name in ("wq", "wk"))
    h = h + matmul(seen_by(q, k, matmul(a, w["wv"]).reshape(h.shape[0], -1, HEAD)), w["wo"])
    b = normed(h)
    gate = jnp.dot(b, w["w_gate"], preferred_element_type=jnp.float32)
    up = jnp.dot(b, w["w_up"], preferred_element_type=jnp.float32)
    return h + matmul((jax.nn.silu(gate) * up).astype(jnp.bfloat16), w["w_down"])


def adamw(w, m, v, g):
    m = 0.9 * m + 0.1 * g
    v = 0.95 * v + 0.05 * g * g
    step = m * lax.rsqrt(v + 1e-8) + 0.1 * w
    return (w - 0.02 * step).astype(jnp.bfloat16), m, v


def clipped(gradients, sum_of_squares, count):
    factor = jnp.minimum(1.0, 0.5 * lax.rsqrt(sum_of_squares / count + 1e-30))
    return [g * factor for g in gradients]


def stack(weights, h):
    return lax.scan(lambda h, w: (layer(h, w), None), h, weights)[0]


def reference(x, dy, wq, wk, wv, wo, w_gate, w_up, w_down, m_wq, m_wk, m_wv, m_wo, m_w_gate, m_w_up, m_w_down, v_wq, v_wk, v_wv, v_wo, v_w_gate, v_w_up, v_w_down):
    weights = dict(zip(NAMES, (wq, wk, wv, wo, w_gate, w_up, w_down), strict=True))

    def take(so_far, sequence):
        h, by_y = sequence
        _, back = jax.vjp(stack, weights, h)
        by_weights, by_h = back(by_y)
        return jax.tree.map(lambda total, term: total + term.astype(jnp.float32), so_far, by_weights), by_h

    none_yet = {name: jnp.zeros(w.shape, jnp.float32) for name, w in weights.items()}
    by_weights, by_x = lax.scan(take, none_yet, (x, dy))
    gradients = [by_weights[name].astype(jnp.bfloat16).astype(jnp.float32) for name in NAMES]
    gradients = clipped(gradients, sum(jnp.sum(g * g) for g in gradients), sum(g.size for g in gradients))
    first = (m_wq, m_wk, m_wv, m_wo, m_w_gate, m_w_up, m_w_down)
    second = (v_wq, v_wk, v_wv, v_wo, v_w_gate, v_w_up, v_w_down)
    new = [adamw(weights[name].astype(jnp.float32), m, v, g) for name, m, v, g in zip(NAMES, first, second, gradients, strict=True)]
    return tuple(one[which] for which in range(3) for one in new)
```

```python
import functools
import math

import jax
import jax.numpy as jnp
import numpy as np
from jax import lax
from jax.experimental import pallas as pl
from jax.experimental.pallas import tpu as pltpu
from jax.sharding import PartitionSpec as P

HEAD = 128
THETA = 10000
NAMES = ("wq", "wk", "wv", "wo", "w_gate", "w_up", "w_down")
NEG = -1e30
LOG2E = 1.4426950408889634
BF = jnp.bfloat16
F32 = jnp.float32
VMEM = 67_043_328
ROWS = 512
ANY = pl.BlockSpec(memory_space=pl.ANY)
ONE = pl.Buffered(1)


def _dot(ca, cb, a, b):
    return lax.dot_general(a, b, (((ca,), (cb,)), ((), ())), preferred_element_type=F32)


_nn, _nt, _tn = (functools.partial(_dot, *c) for c in ((1, 0), (1, 1), (0, 0)))


def _cols(n, size=HEAD):
    return slice(n * size, n * size + size)


def _zero(*refs):
    for ref in refs:
        ref[...] = jnp.zeros(ref.shape, F32)


def _bf(*shape):
    return jax.ShapeDtypeStruct(shape, BF)


def _f32(*shape):
    return jax.ShapeDtypeStruct(shape, F32)


def _params(**more):
    return pltpu.CompilerParams(vmem_limit_bytes=VMEM, **more)


def _norm(h):
    wide = h.astype(F32)
    scale = lax.rsqrt(jnp.mean(wide * wide, -1, keepdims=True) + 1e-6)
    return wide * scale, scale


def _norm_back(xhat, scale, by):
    return scale * (by - xhat * jnp.mean(xhat * by, -1, keepdims=True))


def _tables(tokens, rows):
    half = HEAD // 2
    freq = THETA ** (-np.arange(half) / half)
    freq, sign = np.concatenate([freq, freq]), np.concatenate([-np.ones(half), np.ones(half)])

    def of(places):
        angle = places[:, None] * freq
        return [np.asarray(x, np.float32) for x in (np.cos(angle), np.sin(angle) * sign)]

    return of(np.arange(0, tokens, rows)), of(np.arange(rows))


def _turns(i, refs):
    ca, sa = refs[0][pl.ds(i, 1), :], refs[1][pl.ds(i, 1), :]
    cb, sb = refs[2][...], refs[3][...]
    return ca * cb - sa * sb, sa * cb + ca * sb


def _turn(t, cos, sin):
    return (t * cos + pltpu.roll(t, HEAD // 2, 1) * sin).astype(BF)


def _turn_back(t, cos, sin):
    return (t * cos - pltpu.roll(t, HEAD // 2, 1) * sin).astype(BF)


def _cost(flops, nbytes):
    return pl.CostEstimate(flops=int(flops), transcendentals=0, bytes_accessed=int(nbytes))


def _rows(width, rows=ROWS):
    return pl.BlockSpec((rows, width), lambda i: (i, 0))


def _whole(a):
    return pl.BlockSpec(a.shape, lambda i: (0,) * a.ndim, pipeline_mode=ONE)


def _of_layer(w, number):
    return pl.BlockSpec((1, *w.shape[1:]), lambda i: (number, 0, 0), pipeline_mode=ONE)


def _qkv_kernel(h_ref, wq_ref, wk_ref, wv_ref, ca, sa, cb, sb, q_ref, k_ref, v_ref):
    cos, sin = _turns(pl.program_id(0), (ca, sa, cb, sb))
    a = _norm(h_ref[...])[0].astype(BF)
    for w_ref, out in ((wq_ref, q_ref), (wk_ref, k_ref)):
        for at in range(0, w_ref.shape[2], 256):
            t = _nn(a, w_ref[0, :, at : at + 256]).astype(BF).astype(F32)
            for n in range(0, 256, HEAD):
                out[:, at + n : at + n + HEAD] = _turn(t[:, n : n + HEAD], cos, sin)
    v_ref[...] = _nn(a, wv_ref[0]).astype(BF)


def qkv_forward(h, wq, wk, wv, number):
    s, d = h.shape
    (ca, sa), (cb, sb) = _tables(s, ROWS)
    outs = [wq.shape[2], wk.shape[2], wv.shape[2]]
    return pl.pallas_call(
        _qkv_kernel,
        grid=(s // ROWS,),
        in_specs=[_rows(d), *(_of_layer(w, number) for w in (wq, wk, wv)), *(_whole(t) for t in (ca, sa, cb, sb))],
        out_specs=[_rows(n) for n in outs],
        out_shape=[_bf(s, n) for n in outs],
        compiler_params=_params(),
        cost_estimate=_cost(2 * s * d * sum(outs), 2 * s * (d + sum(outs)) + 2 * d * sum(outs)),
        name="qkv_forward",
    )(h, wq, wk, wv, ca, sa, cb, sb)


def _hidden(bk, bq, shift):
    return lax.broadcasted_iota(jnp.int32, (bk, bq), 1) >= lax.broadcasted_iota(jnp.int32, (bk, bq), 0) + shift


def _attend_kernel(q_ref, k_ref, v_ref, o_ref, lse_ref, top_s, mix_s, *, bk, group):
    bq, width = q_ref.shape
    heads = width // HEAD
    iq = pl.program_id(0)
    scale = HEAD**-0.5
    e = scale * LOG2E
    ones = jnp.ones((8, bk), BF)
    top_s[...] = jnp.full(top_s.shape, NEG, F32)
    _zero(mix_s)

    def block(j, first):
        here = pl.ds(pl.multiple_of(j * bk, bk), bk)
        at = first or 0
        kept = None if first is None else _hidden(bk, bq - at, 0)
        scores = []
        for n in range(heads):
            g = n // group
            scores.append(_nt(k_ref[here, _cols(g)], q_ref[at:, _cols(n)]))
        weights, keeps = [], []
        for n, s in enumerate(scores):
            if first is not None:
                s = jnp.where(kept, s, 2 * NEG)
            old = top_s[n : n + 1, at:]
            top = jnp.maximum(old, s.max(axis=0, keepdims=True))
            top_s[n : n + 1, at:] = top
            weights.append(jnp.exp2((s - top) * e).astype(BF))
            keeps.append(jnp.exp2((old - top) * e))
        values = [jnp.concatenate([v_ref[here, _cols(g)].T, ones], axis=0) for g in range(heads // group)]
        for n, (p, keep) in enumerate(zip(weights, keeps)):
            mix_s[n, :, at:] = mix_s[n, :, at:] * keep + _nn(values[n // group], p)

    per = bq // bk
    lax.fori_loop(0, iq * per, lambda j, _: block(j, None), None)
    for n in range(per):
        block(iq * per + n, n * bk)
    for n in range(heads):
        total = mix_s[n, HEAD : HEAD + 1, :]
        o_ref[:, _cols(n)] = (mix_s[n, :HEAD, :] * (1 / total)).T.astype(BF)
        lse_ref[n : n + 1, :] = top_s[n : n + 1, :] * e + jnp.log2(total)


def attend(q, k, v, bq=512, bk=512):
    s, width = q.shape
    heads, group = width // HEAD, width // k.shape[1]
    pad = -(-heads // 8) * 8
    return pl.pallas_call(
        functools.partial(_attend_kernel, bk=bk, group=group),
        grid=(s // bq,),
        in_specs=[_rows(width, bq), _whole(k), _whole(v)],
        out_specs=[_rows(width, bq), pl.BlockSpec((pad, bq), lambda i: (0, i))],
        out_shape=[_bf(s, width), _f32(pad, s)],
        scratch_shapes=[pltpu.VMEM((pad, bq), F32), pltpu.VMEM((heads, HEAD + 8, bq), F32)],
        compiler_params=_params(),
        cost_estimate=_cost(2 * s * s * width, 4 * s * width),
        name="attend",
    )(q, k, v)


def _attend_back_kernel(q_ref, k_ref, v_ref, do_ref, lse_ref, delta_ref, dq_ref, dk_ref, dv_ref, dq_s, dk_s, dv_s, *, bk, group):
    bq, width = q_ref.shape
    heads = width // HEAD
    iq = pl.program_id(0)
    scale = HEAD**-0.5
    e = scale * LOG2E

    @pl.when(iq == 0)
    def _():
        _zero(dk_s, dv_s)

    _zero(dq_s)

    def block(j, first):
        here = pl.ds(pl.multiple_of(j * bk, bk), bk)
        at = first or 0
        kept = None if first is None else _hidden(bk, bq - at, 0)
        scores, dps = [], []
        for n in range(heads):
            g = n // group
            scores.append(_nt(k_ref[here, _cols(g)], q_ref[at:, _cols(n)]))
            dps.append(_nt(v_ref[here, _cols(g)], do_ref[at:, _cols(n)]))
        for n in range(heads):
            g = n // group
            p = jnp.exp2(scores[n] * e - lse_ref[n : n + 1, at:])
            if first is not None:
                p = jnp.where(kept, p, 0.0)
            ds = (p * (dps[n] - delta_ref[n : n + 1, at:])).astype(BF)
            dv_s[g, here, :] += _nn(p.astype(BF), do_ref[at:, _cols(n)])
            dk_s[g, here, :] += _nn(ds, q_ref[at:, _cols(n)])
            dq_s[n, :, at:] += _nn(k_ref[here, _cols(g)].T, ds)

    per = bq // bk
    lax.fori_loop(0, iq * per, lambda j, _: block(j, None), None)
    for n in range(per):
        block(iq * per + n, n * bk)
    for n in range(heads):
        dq_ref[:, _cols(n)] = (dq_s[n] * scale).T.astype(BF)

    @pl.when(iq == pl.num_programs(0) - 1)
    def _():
        for g in range(heads // group):
            dk_ref[:, _cols(g)] = (dk_s[g] * scale).astype(BF)
            dv_ref[:, _cols(g)] = dv_s[g].astype(BF)


def attend_back(q, k, v, do, lse, delta, bq=512, bk=512):
    s, width = q.shape
    heads, group = width // HEAD, width // k.shape[1]
    pad = lse.shape[0]
    stats = pl.BlockSpec((pad, bq), lambda i: (0, i))
    return pl.pallas_call(
        functools.partial(_attend_back_kernel, bk=bk, group=group),
        grid=(s // bq,),
        in_specs=[_rows(width, bq), _whole(k), _whole(v), _rows(width, bq), stats, stats],
        out_specs=[_rows(width, bq), _whole(k), _whole(v)],
        out_shape=[_bf(s, width), jax.ShapeDtypeStruct(k.shape, BF), jax.ShapeDtypeStruct(v.shape, BF)],
        scratch_shapes=[pltpu.VMEM((heads, HEAD, bq), F32), pltpu.VMEM((heads // group, s, HEAD), F32), pltpu.VMEM((heads // group, s, HEAD), F32)],
        compiler_params=_params(),
        cost_estimate=_cost(5 * s * s * width, 8 * s * width),
        name="attend_back",
    )(q, k, v, do, lse, delta)


def _feed_kernel(o_ref, h_ref, wo_ref, wg_ref, wu_ref, wd_ref, mid_ref, out_ref, gate_ref, up_ref, p_s, *, tile):
    mid = h_ref[...] + _nn(o_ref[...], wo_ref[0]).astype(BF)
    mid_ref[...] = mid
    b = _norm(mid)[0].astype(BF)
    for at in range(0, wg_ref.shape[2], tile):
        here = slice(at, at + tile)
        gate, up = _nn(b, wg_ref[0, :, here]), _nn(b, wu_ref[0, :, here])
        gate_ref[:, here] = gate
        up_ref[:, here] = up
        p_s[:, here] = (gate * jax.nn.sigmoid(gate) * up).astype(BF)
    out_ref[...] = mid + _nn(p_s[...], wd_ref[0]).astype(BF)


def feed_forward(o, h, wo, wg, wu, wd, number, rows=256, tile=768):
    s, d = h.shape
    ff = wg.shape[2]
    return pl.pallas_call(
        functools.partial(_feed_kernel, tile=tile),
        grid=(s // rows,),
        in_specs=[_rows(o.shape[1], rows), _rows(d, rows), *(_of_layer(w, number) for w in (wo, wg, wu, wd))],
        out_specs=[_rows(d, rows), _rows(d, rows), _rows(ff, rows), _rows(ff, rows)],
        out_shape=[_bf(s, d), _bf(s, d), _f32(s, ff), _f32(s, ff)],
        scratch_shapes=[pltpu.VMEM((rows, ff), BF)],
        compiler_params=_params(),
        cost_estimate=_cost(2 * s * d * (d + 3 * ff), 8 * s * ff + 8 * s * d),
        name="feed_forward",
    )(o, h, wo, wg, wu, wd)


def _feed_back_kernel(*refs, tile, fresh, steps):
    if fresh:
        o_ref, h_ref, dy_ref, wo_ref, wg_ref, wu_ref, wd_ref, by_ref, do_ref, delta_ref, g_ref, acc, p_s, dg_s, du_s, stage, sem = refs
        mid = h_ref[...] + _nn(o_ref[...], wo_ref[0]).astype(BF)
    else:
        o_ref, mid_ref, dy_ref, gate_ref, up_ref, wo_ref, wg_ref, wu_ref, wd_ref, by_ref, do_ref, delta_ref, g_ref, acc, p_s, dg_s, du_s, stage, sem, gu_s, gu_sem = refs
        mid = mid_ref[...]
    i = pl.program_id(0)
    rows, d = dy_ref.shape
    ff = wg_ref.shape[2]
    tiles = ff // tile

    if not fresh:

        def fetch(n, slot):
            there = (pl.ds(pl.multiple_of(lax.div(n, tiles) * rows, rows), rows), pl.ds(pl.multiple_of(lax.rem(n, tiles) * tile, 128), tile))
            return [pltpu.make_async_copy(ref.at[there], gu_s.at[slot, w], gu_sem.at[slot, w]) for w, ref in enumerate((gate_ref, up_ref))]

        @pl.when(i == 0)
        def _():
            for c in fetch(0, 0):
                c.start()

    @pl.when(i == 0)
    def _():
        _zero(acc)

    dy = dy_ref[...]
    xhat, scale = _norm(mid)
    b = xhat.astype(BF)
    for f in range(tiles):
        here = _cols(f, tile)
        if fresh:
            gate, up = _nn(b, wg_ref[0, :, here]), _nn(b, wu_ref[0, :, here])
        else:
            n = i * tiles + f
            slot = lax.rem(n, 2)

            @pl.when(n + 1 < steps * tiles)
            def _():
                for c in fetch(n + 1, 1 - slot):
                    c.start()

            for c in fetch(n, slot):
                c.wait()
            gate, up = gu_s[slot, 0], gu_s[slot, 1]
        dp = _nt(dy, wd_ref[0, here, :]).astype(BF).astype(F32)
        sig = jax.nn.sigmoid(gate)
        silu = gate * sig
        p_s[:, here] = (silu * up).astype(BF)
        du_s[:, here] = (dp * silu).astype(BF)
        dg_s[:, here] = (dp * up * (sig * (1 + gate * (1 - sig)))).astype(BF)
    db = (_nt(dg_s[...], wg_ref[0]) + _nt(du_s[...], wu_ref[0])).astype(BF).astype(F32)
    by = dy + _norm_back(xhat, scale, db).astype(BF)
    by_ref[...] = by
    do = _nt(by, wo_ref[0]).astype(BF)
    do_ref[...] = do
    both = do.astype(F32) * o_ref[...].astype(F32)
    for n in range(d // HEAD):
        delta_ref[n : n + 1, :] = both[:, _cols(n)].T.sum(axis=0, keepdims=True)
    bt = b.T
    for f in range(tiles):
        here = _cols(f, tile)
        acc[:, here] += _nn(bt, dg_s[:, here])
        acc[:, ff + f * tile : ff + (f + 1) * tile] += _nn(bt, du_s[:, here])
    for f in range(ff // d):
        acc[:, 2 * ff + f * d : 2 * ff + (f + 1) * d] += _tn(p_s[:, _cols(f, d)], dy)

    @pl.when(i == steps - 1)
    def _():
        part = stage.shape[1]

        def put(n):
            return pltpu.make_async_copy(stage.at[lax.rem(n, 2)], g_ref.at[pl.ds(pl.multiple_of(n * part, part), part), :], sem.at[lax.rem(n, 2)])

        def out(n, _):
            @pl.when(n >= 2)
            def _():
                put(n - 2).wait()

            stage[lax.rem(n, 2)] = acc[pl.ds(pl.multiple_of(n * part, part), part), :].astype(BF)
            put(n).start()

        lax.fori_loop(0, d // part, out, None)
        for n in range(d // part - 2, d // part):
            put(n).wait()


def feed_back(o, h, dy, weights, number, kept=None, rows=ROWS, tile=768):
    s, d = h.shape
    wo, wg, wu, wd = weights
    ff = wg.shape[2]
    fresh = kept is None
    row = _rows(d, rows)
    out_shape = [_bf(s, d), _bf(s, d), _f32(8, s), _bf(d, 3 * ff)]
    scratch = [pltpu.VMEM((d, 3 * ff), F32), *(pltpu.VMEM((rows, ff), BF) for _ in range(3)), pltpu.VMEM((2, 64, 3 * ff), BF), pltpu.SemaphoreType.DMA((2,))]
    if not fresh:
        scratch += [pltpu.VMEM((2, 2, rows, tile), F32), pltpu.SemaphoreType.DMA((2, 2))]
    return pl.pallas_call(
        functools.partial(_feed_back_kernel, tile=tile, fresh=fresh, steps=s // rows),
        grid=(s // rows,),
        in_specs=[row, row, row, *([] if fresh else [ANY, ANY]), *(_of_layer(w, number) for w in weights)],
        out_specs=[row, row, pl.BlockSpec((8, rows), lambda i: (0, i)), ANY],
        out_shape=out_shape,
        scratch_shapes=scratch,
        compiler_params=_params(),
        cost_estimate=_cost(2 * s * d * (2 * d + (8 if fresh else 6) * ff), 8 * s * ff + 8 * s * d),
        name="feed_back",
    )(o, h, dy, *([] if fresh else kept), *weights)


def _qkv_back_kernel(h_ref, by_ref, o_ref, dq_ref, dk_ref, dv_ref, wq_ref, wk_ref, wv_ref, ca, sa, cb, sb, *rest, steps, deep):
    out_ref, g_ref, acc, t_s = rest if deep else (None, *rest)
    i = pl.program_id(0)
    cos, sin = _turns(i, (ca, sa, cb, sb))
    d = h_ref.shape[1]
    nq, nk = dq_ref.shape[1], dk_ref.shape[1]
    for ref, base in ((dq_ref, 0), (dk_ref, nq)):
        for n in range(0, ref.shape[1], HEAD):
            t_s[:, base + n : base + n + HEAD] = _turn_back(ref[:, n : n + HEAD].astype(F32), cos, sin)
    t_s[:, nq + nk :] = dv_ref[...]

    @pl.when(i == 0)
    def _():
        _zero(acc)

    xhat, scale = _norm(h_ref[...])
    at = xhat.astype(BF).T
    wide = nq + 2 * nk
    acc[:, :wide] += _nn(at, t_s[...])
    acc[:, wide:] += _tn(o_ref[...], by_ref[...])
    if deep:
        da = _nt(t_s[:, :nq], wq_ref[0]) + _nt(t_s[:, nq : nq + nk], wk_ref[0]) + _nt(t_s[:, nq + nk :], wv_ref[0])
        out_ref[...] = by_ref[...] + _norm_back(xhat, scale, da.astype(BF).astype(F32)).astype(BF)

    @pl.when(i == steps - 1)
    def _():
        g_ref[...] = acc[...].astype(BF)


def qkv_back(h, by, o, dq, dk, dv, wq, wk, wv, number, deep):
    s, d = h.shape
    (ca, sa), (cb, sb) = _tables(s, ROWS)
    nq, nk = dq.shape[1], dk.shape[1]
    wide = nq + 2 * nk + d
    g_shape = _bf(o.shape[1], wide)
    return pl.pallas_call(
        functools.partial(_qkv_back_kernel, steps=s // ROWS, deep=deep),
        grid=(s // ROWS,),
        in_specs=[_rows(d), _rows(d), _rows(nq), _rows(nq), _rows(nk), _rows(nk), *(_of_layer(w, number) for w in (wq, wk, wv)),
                  *(_whole(t) for t in (ca, sa, cb, sb))],
        out_specs=[*([_rows(d)] if deep else []), _whole(g_shape)],
        out_shape=[*([_bf(s, d)] if deep else []), g_shape],
        scratch_shapes=[pltpu.VMEM((d, wide), F32), pltpu.VMEM((ROWS, nq + 2 * nk), BF)],
        compiler_params=_params(),
        cost_estimate=_cost(2 * s * d * wide * (2 if deep else 1), 12 * s * d),
        name="qkv_back",
    )(h, by, o, dq, dk, dv, wq, wk, wv, ca, sa, cb, sb)


def gradients(x, dy, weights):
    wq, wk, wv, wo, wg, wu, wd = weights
    layers = wq.shape[0]
    kept = []
    h = x
    for n in range(layers):
        q, k, v = qkv_forward(h, wq, wk, wv, n)
        o, lse = attend(q, k, v)
        if n < layers - 1:
            mid, out, gate, up = feed_forward(o, h, wo, wg, wu, wd, n)
            kept.append((h, q, k, v, o, lse, mid, gate, up))
            h = out
        else:
            kept.append((h, q, k, v, o, lse))
    by = dy
    result = [None] * layers
    for n in reversed(range(layers)):
        h, q, k, v, o, lse, *rest = kept[n]
        if rest:
            by, do, delta, feed = feed_back(o, rest[0], by, (wo, wg, wu, wd), n, kept=rest[1:])
        else:
            by, do, delta, feed = feed_back(o, h, by, (wo, wg, wu, wd), n)
        dq, dk, dv = attend_back(q, k, v, do, lse, delta)
        *back, proj = qkv_back(h, by, o, dq, dk, dv, wq, wk, wv, n, deep=n > 0)
        if back:
            by = back[0]
        result[n] = (feed, proj)
    return result


AXES = ((8, 4, 2), (4, 2, 8), (2, 8, 4))
CORE = 1
SIXTEENTHS = 16
MESH = pl.DeviceIdType.MESH


def _bit(stride):
    return lax.rem(lax.div(lax.axis_index("dp"), stride), 2)


def _peer(stride):
    return {"dp": lax.axis_index("dp") + stride * (1 - 2 * _bit(stride))}


def _greet(peers):
    barrier = pltpu.get_barrier_semaphore()
    for peer in peers:
        pl.semaphore_signal(barrier, inc=1, device_id=peer, device_id_type=MESH)
    pl.semaphore_wait(barrier, len(peers))


def _ds(at, size, unit=16):
    return pl.ds(pl.multiple_of(at, unit), size)


def _send(src, dst, sems, peer):
    return pltpu.make_async_remote_copy(src_ref=src, dst_ref=dst, send_sem=sems[0], recv_sem=sems[1], device_id=peer, device_id_type=MESH)


class Scatter:
    def __init__(self, g_ref, out_ref, bufs, local_sem, send_sem, recv_sem):
        self.g, self.out, self.local, self.sends, self.recvs = g_ref, out_ref, local_sem, send_sem, recv_sem
        self.own, self.r0, self.r1, self.r2, self.r3, self.t1, self.t2, self.t3, self.fin = bufs
        self.width = g_ref.shape[1]
        self.third = g_ref.shape[0] // 3
        self.part = self.third // SIXTEENTHS

    @staticmethod
    def scratch(rows, width):
        n = rows // 3 // SIXTEENTHS
        sizes = [8 * n, 8 * n, 4 * n, 2 * n, n, 4 * n, 2 * n, n, n]
        return [*(pltpu.VMEM((3, size, width), BF) for size in sizes), pltpu.SemaphoreType.DMA((4,)), pltpu.SemaphoreType.DMA((3, 5)), pltpu.SemaphoreType.DMA((3, 5))]

    def _sems(self, t, k):
        return self.sends.at[t, k], self.recvs.at[t, k]

    def _bits(self, t):
        return [_bit(s) for s in AXES[t]]

    def _core(self, t, late):
        n, b = self.part, self._bits(t)[0]
        at = 4 * n * (b if late else 1 - b)
        there = t * self.third + 8 * n * (1 - _bit(CORE)) + at
        return _send(self.g.at[_ds(there, 4 * n), :], self.r0.at[t, _ds(at, 4 * n), :], self._sems(t, int(late)), _peer(CORE))

    def _mine(self, t):
        n = self.part
        return pltpu.make_async_copy(self.g.at[_ds(t * self.third + 8 * n * _bit(CORE), 8 * n), :], self.own.at[t], self.local.at[t])

    def _halving(self, t, k):
        src, dst = ((self.t1, self.r1), (self.t2, self.r2), (self.t3, self.r3))[k]
        return _send(src.at[t], dst.at[t], self._sems(t, 2 + k), _peer(AXES[t][k]))

    def start(self):
        for late in (False, True):
            for t in range(3):
                self._core(t, late).start()
                if not late:
                    self._mine(t).start()

    def _add(self, t, dst, at, size, others):
        wide = 256

        def add(j, _):
            here = pl.ds(pl.multiple_of(j * wide, wide), wide)
            total = self.own[t, _ds(at, size), here].astype(F32) + self.r0[t, _ds(at, size), here].astype(F32)
            for ref, first in others:
                total += ref[t, _ds(first, size), here].astype(F32)
            dst[t, :, here] = total.astype(BF)

        lax.fori_loop(0, self.width // wide, add, None)

    def halve(self, k, thirds=range(3)):
        n = self.part
        for t in thirds:
            b1, b2, b3 = self._bits(t)
            if k == 0:
                self._mine(t).wait()
                self._core(t, False).wait()
                self._add(t, self.t1, 4 * n * (1 - b1), 4 * n, ())
            elif k == 1:
                self._core(t, True).wait()
                self._halving(t, 0).wait()
                self._add(t, self.t2, 4 * n * b1 + 2 * n * (1 - b2), 2 * n, ((self.r1, 2 * n * (1 - b2)),))
            else:
                self._halving(t, 1).wait()
                self._add(t, self.t3, 4 * n * b1 + 2 * n * b2 + n * (1 - b3), n, ((self.r1, 2 * n * b2 + n * (1 - b3)), (self.r2, n * (1 - b3))))
            self._halving(t, k).start()

    def finish(self):
        n = self.part
        for t in range(3):
            b1, b2, b3 = self._bits(t)
            self._halving(t, 2).wait()
            self._add(t, self.fin, 4 * n * b1 + 2 * n * b2 + n * b3, n, ((self.r1, 2 * n * b2 + n * b3), (self.r2, n * b3), (self.r3, 0)))
        copy = pltpu.make_async_copy(self.fin, self.out, self.local.at[3])
        copy.start()
        copy.wait()


def _scatter_kernel(g_ref, out_ref, *rest):
    work = Scatter(g_ref, out_ref, rest[:9], *rest[9:])
    _greet([_peer(s) for s in (1, 2, 4, 8)])
    work.start()
    for k in range(3):
        work.halve(k)
    work.finish()


def reduce_scatter(g, collective_id):
    rows, width = g.shape
    return pl.pallas_call(
        _scatter_kernel,
        in_specs=[ANY],
        out_specs=ANY,
        out_shape=_bf(3, rows // 3 // SIXTEENTHS, width),
        scratch_shapes=Scatter.scratch(rows, width),
        compiler_params=_params(collective_id=collective_id, has_side_effects=True),
        name="reduce_scatter",
    )(g)


class Gather:
    def __init__(self, own_ref, all_ref, local_sem, send_sem, recv_sem):
        self.own, self.all, self.local, self.sends, self.recvs = own_ref, all_ref, local_sem, send_sem, recv_sem

    @staticmethod
    def scratch():
        return [pltpu.SemaphoreType.DMA((3,)), pltpu.SemaphoreType.DMA((3, 7)), pltpu.SemaphoreType.DMA((3, 7))]

    def _block(self, t, k, theirs):
        bits = [_bit(CORE), *(_bit(s) for s in AXES[t])]
        if theirs:
            bits[3 - k] = 1 - bits[3 - k]
        at = 8 * bits[0]
        for n, b in zip((4, 2, 1), bits[1:], strict=True):
            if n >= 2**k:
                at = at + n * b
        return at, 2**k

    def _copy(self, t, src, at, count, k, stride):
        return _send(src, self.all.at[t, pl.ds(at, count)], (self.sends.at[t, k], self.recvs.at[t, k]), _peer(stride))

    def _axis(self, t, k):
        at, count = self._block(t, k, False)
        return self._copy(t, self.own.at[pl.ds(t, 1)] if k == 0 else self.all.at[t, pl.ds(at, count)], at, count, k, AXES[t][2 - k])

    def _core(self, t, k):
        at, count = self._block(t, 0, False) if k == 0 else self._block(t, k - 1, True)
        return self._copy(t, self.own.at[pl.ds(t, 1)] if k == 0 else self.all.at[t, pl.ds(at, count)], at, count, 3 + k, CORE)

    def start(self):
        for t in range(3):
            self._axis(t, 0).start()
            self._core(t, 0).start()

    def double(self, k):
        for t in range(3):
            self._axis(t, k).wait_recv()
            if k < 2:
                self._axis(t, k + 1).start()
            self._core(t, k + 1).start()

    def finish(self):
        for t in range(3):
            for k in range(3):
                self._axis(t, k).wait_send()
            for k in range(4):
                self._core(t, k).wait()


def _gather_kernel(*refs, units):
    own, everything, rest = refs[:units], refs[units : 2 * units], refs[2 * units :]
    stages, sems, copied = rest[:units], rest[units : 4 * units], rest[4 * units]
    work = [Gather(stage, a, *sems[3 * n : 3 * n + 3]) for n, (stage, a) in enumerate(zip(stages, everything))]
    loads = [pltpu.make_async_copy(o, s, copied.at[n]) for n, (o, s) in enumerate(zip(own, stages))]
    for c in loads:
        c.start()
    _greet([_peer(s) for s in (1, 2, 4, 8)])
    for c in loads:
        c.wait()
    for g in work:
        g.start()
    puts = []
    for g, s in zip(work, stages):
        for t in range(3):
            at, _ = g._block(t, 0, False)
            puts.append(pltpu.make_async_copy(s.at[pl.ds(t, 1)], g.all.at[t, pl.ds(at, 1)], g.local.at[t]))
            puts[-1].start()
    for c in puts:
        c.wait()
    for k in range(3):
        for g in work:
            g.double(k)
    for g in work:
        g.finish()


def all_gather(parts, collective_id):
    return pl.pallas_call(
        functools.partial(_gather_kernel, units=len(parts)),
        in_specs=[ANY] * len(parts),
        out_specs=[ANY] * len(parts),
        out_shape=[_bf(3, SIXTEENTHS, *p.shape[1:]) for p in parts],
        scratch_shapes=[*(pltpu.VMEM(p.shape, BF) for p in parts), *(s for _ in parts for s in Gather.scratch()), pltpu.SemaphoreType.DMA((len(parts),))],
        compiler_params=_params(collective_id=collective_id, has_side_effects=True),
        name="all_gather",
    )(*parts)


def _size_kernel(*refs, units, devices):
    parts, out_ref, slots, send_sem, recv_sem = refs[:units], *refs[units:]
    me = lax.axis_index("dp")
    others = [lax.rem(me + n, devices) for n in range(1, devices)]
    _greet([{"dp": other} for other in others])
    total = jnp.zeros((8, 128), F32)
    for ref in parts:
        for t in range(3):
            g = ref[t].astype(F32)
            g = g * g
            for at in range(0, g.shape[1], 128):
                for row in range(0, g.shape[0], 8):
                    total += g[row : row + 8, at : at + 128]
    total = jnp.full((8, 128), jnp.sum(total), F32)
    slots[me] = total
    copies = [_send(slots.at[me], slots.at[me], (send_sem.at[n], recv_sem.at[n]), {"dp": other}) for n, other in enumerate(others)]
    for c in copies:
        c.start()
    for c in copies:
        c.wait()
    total = slots[0]
    for n in range(1, devices):
        total += slots[n]
    out_ref[...] = total


def sum_of_squares(parts, devices, collective_id):
    return pl.pallas_call(
        functools.partial(_size_kernel, units=len(parts), devices=devices),
        out_shape=_f32(8, 128),
        scratch_shapes=[pltpu.VMEM((devices, 8, 128), F32), pltpu.SemaphoreType.DMA((devices - 1,)), pltpu.SemaphoreType.DMA((devices - 1,))],
        compiler_params=_params(collective_id=collective_id, has_side_effects=True),
        name="sum_of_squares",
    )(*parts)


def _places(widths, d):
    at, places = 0, []
    for rows, width in widths:
        places.append((at, width, rows // d))
        at += width * (rows // d)
    return places


def _update_kernel(size_ref, *refs, places, layers, rows, steps, slots, count):
    proj, feed = refs[:layers], refs[layers : 2 * layers]
    refs = refs[2 * layers :]
    w_in, m_in, v_in, w_out, m_out, v_out = (refs[7 * n : 7 * n + 7] for n in range(6))
    w_s, m_s, v_s, g_s, wo_s, mo_s, vo_s, in_sem, out_sem = refs[42:]
    d = proj[0].shape[0]
    narrow = proj[0].shape[1]
    factor = jnp.minimum(1.0, 0.5 * lax.rsqrt(size_ref[0:1, 0:1] / count + 1e-30))

    def moves(hbm, buf, layer, row, slot, sem, back):
        for ref, (at, width, blocks) in zip(hbm, places):
            for n in range(blocks):
                there = ref.at[layer, _ds(n * d + row, rows), :]
                here = buf.at[slot, :, at + n * width : at + (n + 1) * width]
                yield pltpu.make_async_copy(here, there, sem) if back else pltpu.make_async_copy(there, here, sem)

    def fetch(layer, row, slot):
        for k, (hbm, buf) in enumerate(((w_in, w_s), (m_in, m_s), (v_in, v_s))):
            for c in moves(hbm, buf, layer, row, slot, in_sem.at[slot, k], False):
                c.start()
        pltpu.make_async_copy(proj[layer].at[_ds(row, rows), :], g_s.at[slot, :, :narrow], in_sem.at[slot, 3]).start()
        pltpu.make_async_copy(feed[layer].at[_ds(row, rows), :], g_s.at[slot, :, narrow:], in_sem.at[slot, 3]).start()

    def wait_all(buf, slot, sem):
        pltpu.make_async_copy(buf.at[slot], buf.at[slot], sem).wait()

    outs = ((w_out, wo_s), (m_out, mo_s), (v_out, vo_s))
    wide = 1280

    def one(layer):
        def at(i, _):
            n = layer * steps + i
            slot = lax.rem(n, slots)

            @pl.when(n >= slots)
            def _():
                for k, (_, buf) in enumerate(outs):
                    wait_all(buf, slot, out_sem.at[slot, k])

            for k, buf in enumerate((w_s, m_s, v_s, g_s)):
                wait_all(buf, slot, in_sem.at[slot, k])

            def part(j, _):
                here = pl.ds(pl.multiple_of(j * wide, 128), wide)
                g = g_s[slot, :, here].astype(F32) * factor
                m = 0.9 * m_s[slot, :, here] + 0.1 * g
                v = 0.95 * v_s[slot, :, here] + 0.05 * g * g
                w = w_s[slot, :, here].astype(F32)
                mo_s[slot, :, here] = m
                vo_s[slot, :, here] = v
                wo_s[slot, :, here] = (w - 0.02 * (m * lax.rsqrt(v + 1e-8) + 0.1 * w)).astype(BF)

            lax.fori_loop(0, g_s.shape[2] // wide, part, None)
            for k, (hbm, buf) in enumerate(outs):
                for c in moves(hbm, buf, layer, i * rows, slot, out_sem.at[slot, k], True):
                    c.start()
            ahead = i + slots

            @pl.when(ahead < steps)
            def _():
                fetch(layer, ahead * rows, slot)

            if layer + 1 < layers:

                @pl.when(ahead >= steps)
                def _():
                    fetch(layer + 1, (ahead - steps) * rows, slot)

        lax.fori_loop(0, steps, at, None)

    for slot in range(slots):
        fetch(0, slot * rows, slot)
    for layer in range(layers):
        one(layer)
    for slot in range(slots):
        for k, (_, buf) in enumerate(outs):
            wait_all(buf, slot, out_sem.at[slot, k])


def update(size, proj, feed, weights, m, v, rows=32, slots=3):
    layers, d = weights[0].shape[:2]
    places = _places([w.shape[1:] for w in (*weights,)], d)
    wide = proj[0].shape[1] + feed[0].shape[1]
    slab = lambda kind: pltpu.VMEM((slots, rows, wide), kind)
    count = sum(w.size for w in weights)
    return pl.pallas_call(
        functools.partial(_update_kernel, places=places, layers=layers, rows=rows, steps=d // rows, slots=slots, count=count),
        in_specs=[pl.BlockSpec(memory_space=pltpu.VMEM), *[ANY] * (2 * layers + 21)],
        out_specs=[ANY] * 21,
        out_shape=[jax.ShapeDtypeStruct(a.shape, a.dtype) for a in (*weights, *m, *v)],
        scratch_shapes=[slab(BF), slab(F32), slab(F32), slab(BF), slab(BF), slab(F32), slab(F32), pltpu.SemaphoreType.DMA((slots, 4)), pltpu.SemaphoreType.DMA((slots, 3))],
        compiler_params=_params(),
        cost_estimate=_cost(20 * count, 22 * count),
        name="update",
    )(size, *proj, *feed, *weights, *m, *v)


def solution(mesh):
    devices = mesh.shape["dp"]

    def step(x, dy, *arrays):
        weights, m, v = (arrays[i : i + 7] for i in (0, 7, 14))
        layers, d = weights[0].shape[:2]
        grads = gradients(x[0], dy[0], weights)
        parts = [reduce_scatter(g, 1 + n) for n, g in enumerate(g for pair in grads for g in pair)]
        size = sum_of_squares(parts, devices, 11)
        full = [a.reshape(d, -1) for a in all_gather(parts, 12)]
        return tuple(update(size, full[1::2], full[0::2], weights, m, v))

    states, all_of = P(("rep", "dp"), None, None), P(None, None, None)
    return jax.shard_map(
        step,
        mesh=mesh,
        in_specs=(states, states) + (all_of,) * 21,
        out_specs=(P("rep", None, None),) * 21,
        check_vma=False,
    )
```

```python
import functools
import math

import jax
import jax.numpy as jnp
import numpy as np
from jax import lax
from jax.experimental import pallas as pl
from jax.experimental.pallas import tpu as pltpu
from jax.sharding import PartitionSpec as P

HEAD = 128
THETA = 10000
NAMES = ("wq", "wk", "wv", "wo", "w_gate", "w_up", "w_down")
NEG = -1e30
LOG2E = 1.4426950408889634
BF = jnp.bfloat16
F32 = jnp.float32
VMEM = 67_043_328
ROWS = 512
ANY = pl.BlockSpec(memory_space=pl.ANY)
ONE = pl.Buffered(1)


def _dot(ca, cb, a, b):
    return lax.dot_general(a, b, (((ca,), (cb,)), ((), ())), preferred_element_type=F32)


_nn, _nt, _tn = (functools.partial(_dot, *c) for c in ((1, 0), (1, 1), (0, 0)))


def _cols(n, size=HEAD):
    return slice(n * size, n * size + size)


def _zero(*refs):
    for ref in refs:
        ref[:] = jnp.zeros(ref.shape, F32)


def _bf(*shape):
    return jax.ShapeDtypeStruct(shape, BF)


def _f32(*shape):
    return jax.ShapeDtypeStruct(shape, F32)


def _params(**more):
    return pltpu.CompilerParams(vmem_limit_bytes=VMEM, **more)


def _norm(h):
    wide = h.astype(F32)
    scale = lax.rsqrt(jnp.mean(wide * wide, -1, keepdims=True) + 1e-6)
    return wide * scale, scale


def _norm_back(xhat, scale, by):
    return scale * (by - xhat * jnp.mean(xhat * by, -1, keepdims=True))


def _tables(tokens, rows):
    half = HEAD // 2
    freq = THETA ** (-np.arange(half) / half)
    freq, sign = np.concatenate([freq, freq]), np.concatenate([-np.ones(half), np.ones(half)])

    def of(places):
        angle = places[:, None] * freq
        return [np.asarray(x, np.float32) for x in (np.cos(angle), np.sin(angle) * sign)]

    return of(np.arange(0, tokens, rows)), of(np.arange(rows))


def _turns(i, refs):
    ca, sa = refs[0][pl.ds(i, 1), :], refs[1][pl.ds(i, 1), :]
    cb, sb = refs[2][:], refs[3][:]
    return ca * cb - sa * sb, sa * cb + ca * sb


def _turn(t, cos, sin):
    return (t * cos + pltpu.roll(t, HEAD // 2, 1) * sin).astype(BF)


def _turn_back(t, cos, sin):
    return (t * cos - pltpu.roll(t, HEAD // 2, 1) * sin).astype(BF)


def _cost(flops, nbytes):
    return pl.CostEstimate(flops=int(flops), transcendentals=0, bytes_accessed=int(nbytes))


def _rows(width, rows=ROWS):
    return pl.BlockSpec((rows, width), lambda i: (i, 0))


def _whole(a):
    return pl.BlockSpec(a.shape, lambda i: (0,) * a.ndim, pipeline_mode=ONE)


def _of_layer(w, number):
    return pl.BlockSpec((1, *w.shape[1:]), lambda i: (number, 0, 0), pipeline_mode=ONE)


def _qkv_kernel(h_ref, wq_ref, wk_ref, wv_ref, ca, sa, cb, sb, q_ref, k_ref, v_ref):
    cos, sin = _turns(pl.program_id(0), (ca, sa, cb, sb))
    a = _norm(h_ref[:])[0].astype(BF)
    for w_ref, out in ((wq_ref, q_ref), (wk_ref, k_ref)):
        for at in range(0, w_ref.shape[2], 256):
            t = _nn(a, w_ref[0, :, at : at + 256]).astype(BF).astype(F32)
            for n in range(0, 256, HEAD):
                out[:, at + n : at + n + HEAD] = _turn(t[:, n : n + HEAD], cos, sin)
    v_ref[:] = _nn(a, wv_ref[0]).astype(BF)


def qkv_forward(h, wq, wk, wv, number):
    s, d = h.shape
    (ca, sa), (cb, sb) = _tables(s, ROWS)
    outs = [wq.shape[2], wk.shape[2], wv.shape[2]]
    return pl.pallas_call(
        _qkv_kernel,
        grid=(s // ROWS,),
        in_specs=[_rows(d), *(_of_layer(w, number) for w in (wq, wk, wv)), *(_whole(t) for t in (ca, sa, cb, sb))],
        out_specs=[_rows(n) for n in outs],
        out_shape=[_bf(s, n) for n in outs],
        compiler_params=_params(),
        cost_estimate=_cost(2 * s * d * sum(outs), 2 * s * (d + sum(outs)) + 2 * d * sum(outs)),
        name="qkv_forward",
    )(h, wq, wk, wv, ca, sa, cb, sb)


def _hidden(bk, bq, shift):
    return lax.broadcasted_iota(jnp.int32, (bk, bq), 1) >= lax.broadcasted_iota(jnp.int32, (bk, bq), 0) + shift


def _attend_kernel(q_ref, k_ref, v_ref, o_ref, lse_ref, top_s, mix_s, *, bk, group):
    bq, width = q_ref.shape
    heads = width // HEAD
    iq = pl.program_id(0)
    scale = HEAD**-0.5
    e = scale * LOG2E
    ones = jnp.ones((8, bk), BF)
    top_s[:] = jnp.full(top_s.shape, NEG, F32)
    _zero(mix_s)

    def block(j, first):
        here = pl.ds(pl.multiple_of(j * bk, bk), bk)
        at = first or 0
        kept = None if first is None else _hidden(bk, bq - at, 0)
        scores = []
        for n in range(heads):
            g = n // group
            scores.append(_nt(k_ref[here, _cols(g)], q_ref[at:, _cols(n)]))
        weights, keeps = [], []
        for n, s in enumerate(scores):
            if first is not None:
                s = jnp.where(kept, s, 2 * NEG)
            old = top_s[n : n + 1, at:]
            top = jnp.maximum(old, s.max(axis=0, keepdims=True))
            top_s[n : n + 1, at:] = top
            weights.append(jnp.exp2((s - top) * e).astype(BF))
            keeps.append(jnp.exp2((old - top) * e))
        values = [jnp.concatenate([v_ref[here, _cols(g)].T, ones], axis=0) for g in range(heads // group)]
        for n, (p, keep) in enumerate(zip(weights, keeps)):
            mix_s[n, :, at:] = mix_s[n, :, at:] * keep + _nn(values[n // group], p)

    per = bq // bk
    lax.fori_loop(0, iq * per, lambda j, _: block(j, None), None)
    for n in range(per):
        block(iq * per + n, n * bk)
    for n in range(heads):
        total = mix_s[n, HEAD : HEAD + 1, :]
        o_ref[:, _cols(n)] = (mix_s[n, :HEAD, :] * (1 / total)).T.astype(BF)
        lse_ref[n : n + 1, :] = top_s[n : n + 1, :] * e + jnp.log2(total)


def attend(q, k, v, bq=512, bk=512):
    s, width = q.shape
    heads, group = width // HEAD, width // k.shape[1]
    pad = -(-heads // 8) * 8
    return pl.pallas_call(
        functools.partial(_attend_kernel, bk=bk, group=group),
        grid=(s // bq,),
        in_specs=[_rows(width, bq), _whole(k), _whole(v)],
        out_specs=[_rows(width, bq), pl.BlockSpec((pad, bq), lambda i: (0, i))],
        out_shape=[_bf(s, width), _f32(pad, s)],
        scratch_shapes=[pltpu.VMEM((pad, bq), F32), pltpu.VMEM((heads, HEAD + 8, bq), F32)],
        compiler_params=_params(),
        cost_estimate=_cost(2 * s * s * width, 4 * s * width),
        name="attend",
    )(q, k, v)


def _feed_kernel(o_ref, h_ref, wo_ref, wg_ref, wu_ref, wd_ref, mid_ref, out_ref, gate_ref, up_ref, bt_ref, p_s):
    mid = h_ref[:] + _nn(o_ref[:], wo_ref[0]).astype(BF)
    mid_ref[:] = mid
    b = _norm(mid)[0].astype(BF)
    bt_ref[:] = b.T
    for n in range(gate_ref.shape[0]):
        here = _cols(n, gate_ref.shape[2])
        gate, up = _nn(b, wg_ref[0, :, here]), _nn(b, wu_ref[0, :, here])
        gate_ref[n] = gate
        up_ref[n] = up
        p_s[:, here] = (gate * jax.nn.sigmoid(gate) * up).astype(BF)
    out_ref[:] = mid + _nn(p_s[:], wd_ref[0]).astype(BF)


def feed_forward(o, h, wo, wg, wu, wd, number, rows=256, width=256):
    s, d = h.shape
    ff = wg.shape[2]
    tile = pl.BlockSpec((ff // width, rows, width), lambda i: (0, i, 0))
    return pl.pallas_call(
        _feed_kernel,
        grid=(s // rows,),
        in_specs=[_rows(o.shape[1], rows), _rows(d, rows), *(_of_layer(w, number) for w in (wo, wg, wu, wd))],
        out_specs=[_rows(d, rows), _rows(d, rows), tile, tile, pl.BlockSpec((d, rows), lambda i: (0, i))],
        out_shape=[_bf(s, d), _bf(s, d), *[_f32(ff // width, s, width)] * 2, _bf(d, s)],
        scratch_shapes=[pltpu.VMEM((rows, ff), BF)],
        compiler_params=_params(),
        cost_estimate=_cost(2 * s * d * (d + 3 * ff), 8 * s * ff + 8 * s * d),
        name="feed_forward",
    )(o, h, wo, wg, wu, wd)


AXES = ((8, 4, 2), (4, 2, 8), (2, 8, 4))
CORE = 1
PART = 16
THIRD = PART * PART
HALF = THIRD // 2
QUARTER = HALF // 2
EIGHTH = QUARTER // 2
THIRDS = range(3)
NEAR = (CORE, *AXES[0])
MESH = pl.DeviceIdType.MESH
DMA = pltpu.SemaphoreType.DMA


def _bit(stride):
    return lax.rem(lax.div(lax.axis_index("dp"), stride), 2)


def _peer(stride):
    return {"dp": lax.axis_index("dp") + stride * (1 - 2 * _bit(stride))}


def _greet(peers):
    barrier = pltpu.get_barrier_semaphore()
    for peer in peers:
        pl.semaphore_signal(barrier, device_id=peer, device_id_type=MESH)
    pl.semaphore_wait(barrier, len(peers))


def _ds(at, size, unit=PART):
    return pl.ds(pl.multiple_of(at, unit), size)


def _send(src, dst, sems, at, peer):
    return pltpu.make_async_remote_copy(src, dst, sems[0].at[at], sems[1].at[at], device_id=peer, device_id_type=MESH)


class Scatter:
    def __init__(self, mine, dst, bufs, sems):
        self.mine, self.dst, self.sems = mine, dst, sems
        self.r0, *self.got, self.sum = bufs

    @staticmethod
    def scratch(width, slots):
        rows = (HALF, QUARTER, EIGHTH, PART, HALF)
        return [pltpu.VMEM((slots, 3, n, width), BF) for n in (THIRD, *rows)] + [DMA((slots, 3, 5))] * 2

    @staticmethod
    def of(scratch, n, dst):
        mine, *bufs, sent, got = [ref.at[lax.rem(n, ref.shape[0])] for ref in scratch]
        return Scatter(mine, dst, bufs, (sent, got))

    def _core(self, t, late):
        b = _bit(AXES[t][0])
        at = QUARTER * (b if late else 1 - b)
        return _send(self.mine.at[t, _ds(HALF * (1 - _bit(CORE)) + at, QUARTER), :], self.r0.at[t, _ds(at, QUARTER), :], self.sems, (t, 3 + late), _peer(CORE))

    def _over(self, t, k):
        size = QUARTER >> k
        return _send(self.sum.at[t, HALF - 2 * size : HALF - size, :], self.got[k].at[t], self.sems, (t, k), _peer(AXES[t][k]))

    def start(self):
        for late in (False, True):
            for t in THIRDS:
                self._core(t, late).start()

    def _add(self, t, k, dst):
        bits = [_bit(stride) for stride in AXES[t]]
        if k < 3:
            bits[k] = 1 - bits[k]
        size = QUARTER >> min(k, 2)
        at = [sum(b * (QUARTER >> n) for n, b in list(enumerate(bits[: k + 1]))[m:]) for m in range(min(k, 2) + 2)]
        total = self.mine[t, _ds(HALF * _bit(CORE) + at[0], size), :].astype(F32) + self.r0[t, _ds(at[0], size), :].astype(F32)
        for n in range(k):
            total += self.got[n][t, _ds(at[n + 1] if n < 2 else 0, size), :].astype(F32)
        dst[:] = total.astype(BF)

    def halve(self, k):
        for t in THIRDS:
            if k < 2:
                self._core(t, bool(k)).wait()
            if k:
                self._over(t, k - 1).wait()
        size = QUARTER >> k
        for t in THIRDS:
            self._add(t, k, self.sum.at[t, HALF - 2 * size : HALF - size, :])
        for t in THIRDS:
            self._over(t, k).start()

    def finish(self):
        for t in THIRDS:
            self._over(t, 2).wait()
        for t in THIRDS:
            self._add(t, 3, self.dst.at[t])


class Gather:
    def __init__(self, own, everything, sems):
        self.own, self.all, self.sems = own, everything, sems

    @staticmethod
    def scratch(own):
        return [pltpu.VMEM(own.shape, BF), DMA((4,)), DMA((3, 9)), DMA((3, 9))]

    def _move(self, t, k, axis=True):
        bits = [_bit(CORE), *(_bit(stride) for stride in AXES[t])]
        over = THIRDS[-1 - min(max(k, 0), 2)]
        if k == 3:
            bits[2] = 1 - bits[2]
        if k >= 0 and not axis:
            bits[1 + over] = 1 - bits[1 + over]
        count = 1 << min(max(k, 0), 1)
        there = self.all.at[t, pl.ds(sum(b * (8 >> n) for n, b in enumerate(bits) if 8 >> n >= count), count)]
        src = there if k > 0 or not axis and k == 0 else self.own.at[pl.ds(t, 1)]
        return _send(src, there, self.sems, (t, k if axis else 5 + k), _peer(AXES[t][over] if axis else CORE))

    def place(self, sem):
        return [pltpu.make_async_copy(self.own.at[pl.ds(t, 1)], self._move(t, -1, False).dst_ref, sem.at[t]) for t in THIRDS]

    def start(self):
        for t in THIRDS:
            self._move(t, 0).start()
            self._move(t, -1, False).start()

    def double(self, k):
        for t in THIRDS:
            self._move(t, k).wait_recv()
            if k == 0:
                self._move(t, 1).start()
            elif k == 1:
                self._move(t, 3).start()
            self._move(t, k, False).start()
        if k == 0:
            for t in THIRDS:
                self._move(t, 2).start()

    def finish(self):
        for t in THIRDS:
            for k in range(4):
                self._move(t, k).wait_send()
                self._move(t, k, False).wait()
            self._move(t, -1, False).wait()


class Gathers:
    def __init__(self, own, everything, scratch):
        self.units = []
        for n, (o, a) in enumerate(zip(own, everything)):
            stage, sem, *sems = scratch[4 * n : 4 * n + 4]
            self.units.append((Gather(stage, a, sems), pltpu.make_async_copy(o, stage, sem.at[3]), sem))

    def start(self):
        for _, load, _ in self.units:
            load.start()
        for g, load, sem in self.units:
            load.wait()
            g.start()
            for c in g.place(sem):
                c.start()

    def double(self, k):
        for g, _, sem in self.units:
            if k == 0:
                for c in g.place(sem):
                    c.wait()
            g.double(k)

    def finish(self):
        for g, *_ in self.units:
            g.finish()

    @staticmethod
    def outs(parts):
        return [_bf(3, PART, *p.shape[1:]) for p in parts]

    @staticmethod
    def scratch(parts):
        return [s for p in parts for s in Gather.scratch(p)]


def _feed_back_kernel(*refs, fresh, number, tiles, guest):
    take = iter(refs)
    some = lambda n: [next(take) for _ in range(n)]
    o_hbm, mid_hbm, dy_hbm, wo_hbm, wg_hbm, wu_hbm, wd_hbm = some(7)
    kept = [] if fresh else some(3)
    guests = some(min(guest, 1))
    by_hbm, do_hbm, delta_ref, own_ref = some(4)
    dy_s, wo_s, wg_s, wu_s, dg_s, du_s, load, pair_sem = some(8)
    room = some(8)
    tile_s = room[0]
    slots = tile_s.shape[0]
    s, d = dy_s.shape
    width = THIRD
    blocks = s // ROWS
    rows = lambda r: _ds(r * ROWS, ROWS)
    halves = [functools.partial(Scatter.halve, k=k) for k in THIRDS]

    def run(copies):
        for c in copies:
            c.start()

    def settle(copies):
        for c in copies:
            c.wait()

    def tell(now, acts):
        for act, back, first, last in acts:
            n = now - back

            @pl.when((n >= first) & (n <= last))
            def _():
                act(Scatter.of(room, n + 2 * guest, own_ref.at[:, n + guest]))

    def acts(last):
        backs = (Scatter.finish, slots), (halves[2], slots - 1), (halves[1], slots - 2), (halves[0], 2), (Scatter.start, 1)
        return [(act, back, -guest, last if back > 2 else tiles - 1) for act, back in backs]

    def row_loads(r, bufs):
        here = rows(r) if fresh else slice(None)
        return [pltpu.make_async_copy(hbm.at[rows(r), :], buf.at[here, :], pair_sem.at[n]) for n, (hbm, buf) in enumerate(zip((o_hbm, mid_hbm), bufs))]

    late_loads = [pltpu.make_async_copy(hbm.at[number], buf, load.at[n]) for n, (hbm, buf) in enumerate(((wo_hbm, wo_s), (wg_hbm, wg_s), (wu_hbm, wu_s)))]

    def tile_phase(wd_s, wd_sem, bt_s, p_s, *more):
        pairs = [(dy_hbm, dy_s)] if fresh else [(dy_hbm, dy_s), (kept[2], bt_s.at[:, :s])]
        pairs += [(ref.at[:, :, _cols(n, d)], tile_s.at[(n + guest) % slots]) for ref in guests for n in range(guest)]
        loads = [pltpu.make_async_copy(*pair, load.at[3 + n]) for n, pair in enumerate(pairs)]

        def down(n):
            slot = lax.rem(n, 2)
            return pltpu.make_async_copy(wd_hbm.at[number, _ds(lax.rem(n, tiles) * width, width), :], wd_s.at[slot], wd_sem.at[slot])

        def fetch(n):
            slot = lax.rem(n, 2)
            return [pltpu.make_async_copy(ref.at[lax.rem(n, tiles)], more[0].at[slot, w], more[1].at[slot, w]) for w, ref in enumerate(kept[:2])]

        run([down(0)] + (row_loads(0, more[1:]) + late_loads + loads if fresh else loads[::-1] + fetch(0)))
        _greet([_peer(stride) for stride in NEAR])
        settle(loads[2:])
        lax.fori_loop(min(1 - guest, 0), 0, lambda now, _: tell(now, acts(0)), None)
        if fresh:
            b_s, *bufs = more
            o_s, mid_s = bufs
            settle(late_loads[:1])

            def prepare(r, _):
                settle(row_loads(r, bufs))
                pl.when(r + 1 < blocks)(lambda: run(row_loads(r + 1, bufs)))
                mid = mid_s[rows(r), :] + _nn(o_s[rows(r), :], wo_s[:]).astype(BF)
                mid_s[rows(r), :] = mid
                b = _norm(mid)[0].astype(BF)
                b_s[rows(r), :] = b
                bt_s[:, _ds(r * ROWS, ROWS, ROWS)] = b.T

            lax.fori_loop(0, blocks, prepare, None)
            settle(late_loads[1:] + loads)
        else:
            settle(loads[:2])
            run(late_loads)

        def tile(i, _):
            tell(i, acts(tiles))
            f = _ds(i * width, width, width)
            settle([down(i)] + fetch(i))
            run([down(i + 1)] + fetch(i + 1))
            wd = wd_s[lax.rem(i, 2)]
            for r in range(blocks):
                here = _cols(r, ROWS)
                if fresh:
                    gate, up = _nn(b_s[here, :], wg_s[:, f]), _nn(b_s[here, :], wu_s[:, f])
                else:
                    gate, up = (more[0][lax.rem(i, 2), w, here, :] for w in range(2))
                dp = _nt(dy_s[here, :], wd).astype(BF).astype(F32)
                sig = jax.nn.sigmoid(gate)
                silu = gate * sig
                p_s[here, :] = (silu * up).astype(BF)
                du_s[here, f] = (dp * silu).astype(BF)
                dg_s[here, f] = (dp * up * (sig * (1 + gate * (1 - sig)))).astype(BF)
            new = tile_s.at[lax.rem(i + 2 * guest, slots)]
            for n, right in enumerate((dg_s[:, f], du_s[:, f])):
                out = _nn(bt_s[:, :s], right).astype(BF)
                for t in THIRDS:
                    new[t, :, _cols(n, width)] = out[_cols(t, THIRD), :]
            out = _tn(p_s[:], dy_s[:]).astype(BF)
            for t in THIRDS:
                new[t, :, 2 * width :] = out[:, _cols(t, width)]

        lax.fori_loop(0, tiles, tile, None)
        settle([down(tiles)] + fetch(tiles))

    def row_phase(by_s, do_s, sem, *bufs):
        def row_stores(r):
            return [pltpu.make_async_copy(buf, hbm.at[rows(r), :], sem.at[n]) for n, (hbm, buf) in enumerate(((by_hbm, by_s), (do_hbm, do_s)))]

        if not fresh:
            settle(late_loads)

        def row(r, _):
            tell(tiles + r, acts(tiles - 2) + [(halves[1 + n], slots - 3 + n, tiles - 1, tiles - 1) for n in (1, 0)])
            here = rows(r)
            part = here if fresh else slice(None)
            if not fresh:
                run(row_loads(r, bufs))
            db = (_nt(dg_s[here, :], wg_s[:]) + _nt(du_s[here, :], wu_s[:])).astype(BF).astype(F32)
            if not fresh:
                settle(row_loads(r, bufs))
            pl.when(r > 0)(lambda: settle(row_stores(r - 1)))
            o_s, mid_s = bufs
            xhat, scale = _norm(mid_s[part, :])
            by = dy_s[here, :] + _norm_back(xhat, scale, db).astype(BF)
            by_s[:] = by
            do = _nt(by, wo_s[:]).astype(BF)
            do_s[:] = do
            run(row_stores(r))
            both = do.astype(F32) * o_s[part, :].astype(F32)
            for n in range(d // HEAD):
                delta_ref[n : n + 1, _ds(r * ROWS, ROWS, ROWS)] = both[:, _cols(n)].T.sum(axis=0, keepdims=True)

        lax.fori_loop(0, blocks, row, None)
        settle(row_stores(blocks - 1))

    vmem = lambda *shape: pltpu.VMEM(shape, BF)
    kinds = [vmem(2, width, d), DMA((2,)), vmem(d, s + HEAD), vmem(s, width)]
    out = [vmem(ROWS, d), vmem(ROWS, d)]
    if fresh:

        def all_phases(*bufs):
            pl.run_scoped(lambda *a: tile_phase(*a, *bufs), *kinds, vmem(s, d))
            pl.run_scoped(lambda *a: row_phase(*a, *bufs), *out, DMA((2,)))

        pl.run_scoped(all_phases, vmem(s, d), vmem(s, d))
    else:
        pl.run_scoped(tile_phase, *kinds, pltpu.VMEM((2, 2, s, width), F32), DMA((2, 2)))
        pl.run_scoped(row_phase, *out, DMA((2,)), *out)
    for n in (tiles - 2, tiles - 1):
        Scatter.of(room, n + 2 * guest, own_ref.at[:, n + guest]).finish()


def feed_back(o, h, dy, weights, number, collective_id, kept=(), guest=(), slots=6):
    s, d = h.shape
    ff = weights[1].shape[2]
    tiles = ff // THIRD
    fresh = not kept
    tiles_in = guest[0].shape[2] // d if guest else 0
    own = _bf(3, tiles_in + tiles, PART, d)
    scratch = [pltpu.VMEM(shape, BF) for shape in ((s, d), *(w.shape[1:] for w in weights[:3]), (s, ff), (s, ff))]
    in_vmem = pl.BlockSpec(memory_space=pltpu.VMEM)
    return pl.pallas_call(
        functools.partial(_feed_back_kernel, fresh=fresh, number=number, tiles=tiles, guest=tiles_in),
        in_specs=[ANY] * (7 + len(kept) + len(guest)),
        out_specs=[ANY, ANY, in_vmem, in_vmem],
        out_shape=[_bf(s, d), _bf(s, d), _f32(8, s), own],
        scratch_shapes=[*scratch, DMA((8,)), DMA((2,)), *Scatter.scratch(d, slots)],
        compiler_params=_params(collective_id=collective_id, has_side_effects=True),
        cost_estimate=_cost(2 * s * d * (2 * d + (8 if fresh else 6) * ff), 8 * s * ff + 8 * s * d),
        name="feed_back",
    )(o, h, dy, *weights, *kept, *guest)


def _attend_back_kernel(q_ref, k_ref, v_ref, do_ref, lse_ref, delta_ref, *rest, bk, group, units, first):
    own, rest = rest[:units], rest[units:]
    dq_ref, dk_ref, dv_ref, *rest = rest
    everything, rest = rest[:units], rest[units:]
    dq_s, dk_s, dv_s, *rest = rest
    work = Gathers([ref.at[:, first:] for ref in own], everything, rest)
    bq, width = q_ref.shape
    heads = width // HEAD
    iq = pl.program_id(0)
    last = pl.num_programs(0) - 1
    scale = HEAD**-0.5
    e = scale * LOG2E

    @pl.when(iq == 0)
    def _():
        _greet([_peer(stride) for stride in NEAR])
        work.start()
        _zero(dk_s, dv_s)

    _zero(dq_s)

    def block(j, first):
        here = _ds(j * bk, bk)
        at = first or 0
        kept = None if first is None else _hidden(bk, bq - at, 0)
        scores, dps = [], []
        for n in range(heads):
            g = n // group
            scores.append(_nt(k_ref[here, _cols(g)], q_ref[at:, _cols(n)]))
            dps.append(_nt(v_ref[here, _cols(g)], do_ref[at:, _cols(n)]))
        for n in range(heads):
            g = n // group
            p = jnp.exp2(scores[n] * e - lse_ref[n : n + 1, at:])
            if first is not None:
                p = jnp.where(kept, p, 0.0)
            ds = (p * (dps[n] - delta_ref[n : n + 1, at:])).astype(BF)
            dv_s[g, here, :] += _nn(p.astype(BF), do_ref[at:, _cols(n)])
            dk_s[g, here, :] += _nn(ds, q_ref[at:, _cols(n)])
            dq_s[n, :, at:] += _nn(k_ref[here, _cols(g)].T, ds)

    per = bq // bk
    lax.fori_loop(0, iq * per, lambda j, _: block(j, None), None)
    for n in THIRDS:
        pl.when(iq == last - 2 + n)(functools.partial(work.double, n))
    for n in range(per):
        block(iq * per + n, n * bk)
    for n in range(heads):
        dq_ref[:, _cols(n)] = (dq_s[n] * scale).T.astype(BF)

    @pl.when(iq == last)
    def _():
        work.double(3)
        for g in range(heads // group):
            dk_ref[:, _cols(g)] = (dk_s[g] * scale).astype(BF)
            dv_ref[:, _cols(g)] = dv_s[g].astype(BF)
        work.finish()


def attend_back(q, k, v, do, lse, delta, parts, first, collective_id, bq=ROWS, bk=ROWS):
    s, width = q.shape
    heads, groups = width // HEAD, k.shape[1] // HEAD
    stats = pl.BlockSpec((lse.shape[0], bq), lambda i: (0, i))
    out = [_bf(*t.shape) for t in (q, k, v)]
    mine = [_bf(3, p.shape[1] - first, *p.shape[2:]) for p in parts]
    return pl.pallas_call(
        functools.partial(_attend_back_kernel, bk=bk, group=heads // groups, units=len(parts), first=first),
        grid=(s // bq,),
        in_specs=[_rows(width, bq), _whole(k), _whole(v), _rows(width, bq), stats, stats, *[ANY] * len(parts)],
        out_specs=[_rows(width, bq), _whole(k), _whole(v), *[ANY] * len(parts)],
        out_shape=[*out, *Gathers.outs(mine)],
        scratch_shapes=[pltpu.VMEM(shape, F32) for shape in ((heads, HEAD, bq), (groups, s, HEAD), (groups, s, HEAD))] + Gathers.scratch(mine),
        compiler_params=_params(collective_id=collective_id, has_side_effects=True),
        cost_estimate=_cost(5 * s * s * width, 8 * s * width),
        name="attend_back",
    )(q, k, v, do, lse, delta, *parts)


def _qkv_back_kernel(h_ref, by_ref, o_ref, dq_ref, dk_ref, dv_ref, wq_ref, wk_ref, wv_ref, ca, sa, cb, sb, *rest, steps, deep):
    out_ref, g_ref, acc, t_s = rest if deep else (None, *rest)
    i = pl.program_id(0)
    cos, sin = _turns(i, (ca, sa, cb, sb))
    d = h_ref.shape[1]
    nq, nk = dq_ref.shape[1], dk_ref.shape[1]
    for ref, base in ((dq_ref, 0), (dk_ref, nq)):
        for n in range(0, ref.shape[1], HEAD):
            t_s[:, base + n : base + n + HEAD] = _turn_back(ref[:, n : n + HEAD].astype(F32), cos, sin)
    t_s[:, nq + nk :] = dv_ref[:]

    @pl.when(i == 0)
    def _():
        _zero(acc)

    xhat, scale = _norm(h_ref[:])
    at = xhat.astype(BF).T
    wide = nq + 2 * nk
    acc[:, :wide] += _nn(at, t_s[:])
    acc[:, wide : wide + d] += _tn(o_ref[:], by_ref[:])
    if deep:
        da = _nt(t_s[:, :nq], wq_ref[0]) + _nt(t_s[:, nq : nq + nk], wk_ref[0]) + _nt(t_s[:, nq + nk :], wv_ref[0])
        out_ref[:] = by_ref[:] + _norm_back(xhat, scale, da.astype(BF).astype(F32)).astype(BF)

    @pl.when(i == steps - 1)
    def _():
        g_ref[:] = acc[:].astype(BF)


def qkv_back(h, by, o, dq, dk, dv, wq, wk, wv, number, deep):
    s, d = h.shape
    (ca, sa), (cb, sb) = _tables(s, ROWS)
    nq, nk = dq.shape[1], dk.shape[1]
    wide = nq + 2 * nk + d
    wide = -(-wide // d) * d
    g_shape = _bf(o.shape[1], wide)
    return pl.pallas_call(
        functools.partial(_qkv_back_kernel, steps=s // ROWS, deep=deep),
        grid=(s // ROWS,),
        in_specs=[_rows(d), _rows(d), _rows(nq), _rows(nq), _rows(nk), _rows(nk), *(_of_layer(w, number) for w in (wq, wk, wv)),
                  *(_whole(t) for t in (ca, sa, cb, sb))],
        out_specs=[*([_rows(d)] if deep else []), _whole(g_shape)],
        out_shape=[*([_bf(s, d)] if deep else []), g_shape],
        scratch_shapes=[pltpu.VMEM((d, wide), F32), pltpu.VMEM((ROWS, nq + 2 * nk), BF)],
        compiler_params=_params(),
        cost_estimate=_cost(2 * s * d * wide * (2 if deep else 1), 12 * s * d),
        name="qkv_back",
    )(h, by, o, dq, dk, dv, wq, wk, wv, ca, sa, cb, sb)


def _settle_kernel(last_ref, *refs, units, devices):
    parts, (size_ref, *alls), (own_s, load, local, slots, *sems) = refs[:units], refs[units : units + 3], refs[units + 3 :]
    sems, room, sems_all = sems[:2], sems[2:10], sems[10:]
    tiles = own_s.shape[1]
    work = [Scatter.of(room, n, own_s.at[:, n]) for n in range(tiles)]
    late, early = (Gather(own, everything, sems_all[2 * n : 2 * n + 2]) for n, (own, everything) in enumerate(zip((own_s, parts[-1].at[:, :tiles]), alls)))
    me = lax.axis_index("dp")
    others = [lax.rem(me + n, devices) for n in range(1, devices)]
    loads = [pltpu.make_async_copy(last_ref.at[:, :, _cols(n, room[0].shape[3])], room[0].at[n], load.at[n]) for n in range(tiles)]
    for c in loads:
        c.start()
    _greet([{"dp": other} for other in others])
    for c, w in zip(loads, work):
        c.wait()
        w.start()
    places = early.place(local.at[0]), late.place(local.at[1])
    early.start()
    for c in places[0]:
        c.start()

    def squares(ref, total):
        def one(n, total):
            g = ref[lax.div(n, ref.shape[1]), lax.rem(n, ref.shape[1])].astype(F32)
            g = g * g
            return total + sum(g[row : row + 8, _cols(at)] for at in range(g.shape[1] // HEAD) for row in (0, 8))

        return lax.fori_loop(0, 3 * ref.shape[1], one, total)

    total = jnp.zeros(size_ref.shape, F32)
    for ref in parts:
        total = squares(ref, total)
    for c in places[0]:
        c.wait()
    for k in THIRDS:
        for w in work:
            w.halve(k)
        early.double(k)
    for w in work:
        w.finish()
    late.start()
    for c in places[1]:
        c.start()
    slots[me] = jnp.full(total.shape, jnp.sum(squares(own_s, total)), F32)
    copies = [_send(slots.at[me], slots.at[me], sems, n, {"dp": other}) for n, other in enumerate(others)]
    for c in copies:
        c.start()
    early.double(3)
    for c in places[1]:
        c.wait()
    for k in THIRDS:
        late.double(k)
    for c in copies:
        c.wait()
    total = slots[0]
    for n in range(1, devices):
        total += slots[n]
    size_ref[:] = total
    late.double(3)
    for g in (early, late):
        g.finish()


def settle(last, parts, devices, collective_id):
    width = parts[-1].shape[3]
    tiles = last.shape[2] // width
    own = _bf(3, tiles, PART, width)
    vmem = pl.BlockSpec(memory_space=pltpu.VMEM)
    return pl.pallas_call(
        functools.partial(_settle_kernel, units=len(parts), devices=devices),
        in_specs=[ANY, *[vmem] * len(parts)],
        out_specs=[vmem, ANY, ANY],
        out_shape=[_f32(8, HEAD), *Gathers.outs([own, own])],
        scratch_shapes=[pltpu.VMEM(own.shape, BF), DMA((tiles,)), DMA((2, 3)), pltpu.VMEM((devices, 8, HEAD), F32), *[DMA((devices,))] * 2,
                        *Scatter.scratch(width, tiles), *[DMA((3, 9))] * 4],
        compiler_params=_params(collective_id=collective_id, has_side_effects=True),
        name="settle",
    )(last, *parts)


NEW = range(3, 6)


def _update_kernel(size_ref, *refs, layers, slots, count):
    proj, feed = refs[:layers], refs[layers : 2 * layers]
    refs = refs[2 * layers :]
    hbm = [refs[7 * n : 7 * n + 7] for n in range(6)]
    flat, deep, gp_s, gf_s, in_sem, g_sem, out_sem = refs[42:48], refs[48:54], *refs[54:]
    rows = flat[0].shape[1]
    sixteenths = rows // PART
    tiles = gf_s.shape[2]
    steps = 3 * PART // sixteenths
    factor = jnp.minimum(1.0, 0.5 * lax.rsqrt(size_ref[0:1, 0:1] / count + 1e-30))
    narrow = sum(ref.shape[2] for ref in hbm[0][:4])

    def moves(k, layer, i, slot):
        sem = out_sem.at[slot, k % 3] if k in NEW else in_sem.at[slot, k]
        at = 0
        for ref in hbm[k][:6]:
            there, here = ref.at[layer, _ds(i * rows, rows), :], flat[k].at[slot, :, at : at + ref.shape[2]]
            yield pltpu.make_async_copy(here, there, sem) if k in NEW else pltpu.make_async_copy(there, here, sem)
            at += ref.shape[2]
        per = PART // sixteenths
        there = hbm[k][6].at[layer, :, _ds(lax.rem(i, per) * rows, rows), _ds(lax.div(i, per) * THIRD, THIRD, THIRD)]
        yield pltpu.make_async_copy(deep[k].at[slot], there, sem) if k in NEW else pltpu.make_async_copy(there, deep[k].at[slot], sem)

    def fetch(layer, i, slot):
        per = PART // sixteenths
        for n, (ref, buf) in enumerate(((proj[layer], gp_s), (feed[layer], gf_s))):
            pltpu.make_async_copy(ref.at[lax.div(i, per), pl.ds(lax.rem(i, per) * sixteenths, sixteenths)], buf.at[slot], g_sem.at[slot, n]).start()
        for k in THIRDS:
            for c in moves(k, layer, i, slot):
                c.start()

    def settled(k, slot):
        sem = out_sem.at[slot, k % 3] if k in NEW else in_sem.at[slot, k]
        for buf in (flat[k], deep[k]):
            pltpu.make_async_copy(buf.at[slot], buf.at[slot], sem).wait()

    def advance(g, bufs, at):
        g = g.astype(F32) * factor
        w, m, v = (buf[at].astype(F32) for buf in bufs[:3])
        m = 0.9 * m + 0.1 * g
        v = 0.95 * v + 0.05 * g * g
        for buf, new in zip(bufs[3:], (w - 0.02 * (m * lax.rsqrt(v + 1e-8) + 0.1 * w), m, v)):
            buf[at] = new.astype(buf.dtype)

    def one(layer):
        def step(i, _):
            n = layer * steps + i
            slot = lax.rem(n, slots)

            @pl.when(n >= slots)
            def _():
                for k in NEW:
                    settled(k, slot)

            for n, buf in enumerate((gp_s, gf_s)):
                pltpu.make_async_copy(buf.at[slot], buf.at[slot], g_sem.at[slot, n]).wait()
            for k in THIRDS:
                settled(k, slot)

            def tile(f, _):
                for n in range(sixteenths):
                    here = _cols(n, PART)
                    for w in range(2):
                        advance(gf_s[slot, n, f, :, _cols(w, THIRD)], flat, (slot, here, _ds(narrow + (w * tiles + f) * THIRD, THIRD, THIRD)))
                    advance(gf_s[slot, n, f, :, 2 * THIRD :], deep, (slot, f, here))

            lax.fori_loop(0, tiles, tile, None)

            def plain(f, _):
                for n in range(sixteenths):
                    across = _ds(f * THIRD, THIRD, THIRD)
                    g = gp_s[slot, n, lax.div(f, 3), :, _ds(lax.rem(f, 3) * THIRD, THIRD, THIRD)]
                    advance(g, flat, (slot, _cols(n, PART), across))

            lax.fori_loop(0, narrow // THIRD, plain, None)
            for k in NEW:
                for c in moves(k, layer, i, slot):
                    c.start()
            ahead = i + slots
            pl.when(ahead < steps)(lambda: fetch(layer, ahead, slot))
            if layer + 1 < layers:
                pl.when(ahead >= steps)(lambda: fetch(layer + 1, ahead - steps, slot))

        lax.fori_loop(0, steps, step, None)

    for slot in range(slots):
        fetch(0, slot, slot)
    for layer in range(layers):
        one(layer)
    for slot in range(slots):
        for k in NEW:
            settled(k, slot)


def update(size, proj, feed, weights, m, v, slots=3, sixteenths=2):
    layers, d, ff = weights[4].shape
    rows = sixteenths * PART
    split = lambda a: a.reshape(layers, -1, THIRD, d)
    state = [a for kind in (weights, m, v) for a in (*kind[:6], split(kind[6]))]
    kinds = (BF, F32, F32) * 2
    flat = [pltpu.VMEM((slots, rows, sum(w.shape[2] for w in weights[:6])), kind) for kind in kinds]
    deep = [pltpu.VMEM((slots, ff // THIRD, rows, THIRD), kind) for kind in kinds]
    grads = [pltpu.VMEM((slots, sixteenths, *g.shape[2:]), BF) for g in (proj[0], feed[0])]
    count = sum(w.size for w in weights)
    new = pl.pallas_call(
        functools.partial(_update_kernel, layers=layers, slots=slots, count=count),
        in_specs=[pl.BlockSpec(memory_space=pltpu.VMEM), *[ANY] * (2 * layers + 21)],
        out_specs=[ANY] * 21,
        out_shape=[jax.ShapeDtypeStruct(a.shape, a.dtype) for a in state],
        scratch_shapes=[*flat, *deep, *grads, DMA((slots, 3)), DMA((slots, 2)), DMA((slots, 3))],
        compiler_params=_params(),
        cost_estimate=_cost(20 * count, 22 * count),
        name="update",
    )(size, *proj, *feed, *state)
    return [a.reshape(old.shape) for a, old in zip(new, (*weights, *m, *v))]


def solution(mesh):
    devices = mesh.shape["dp"]

    def step(x, dy, *arrays):
        weights, m, v = (arrays[i : i + 7] for i in (0, 7, 14))
        wq, wk, wv, *feeds = weights
        layers = wq.shape[0]
        h, kept = x[0], []
        for n in range(layers):
            qkv = qkv_forward(h, wq, wk, wv, n)
            o, lse = attend(*qkv)
            if n < layers - 1:
                mid, out, *rest = feed_forward(o, h, *feeds, n)
                kept.append((h, qkv, o, lse, mid, rest))
                h = out
            else:
                kept.append((h, qkv, o, lse, h, ()))
        by, guest = dy[0], ()
        parts, feed = [], [None] * layers
        for n in reversed(range(layers)):
            h, qkv, o, lse, mid, rest = kept[n]
            by, do, delta, own = feed_back(o, mid, by, feeds, n, 2 * n + 1, rest, guest)
            dq, dk, dv, feed[n] = attend_back(*qkv, do, lse, delta, [own], own.shape[1] - feeds[1].shape[2] // THIRD, 2 * n + 2)
            parts.append(own)
            *back, last = qkv_back(h, by, o, dq, dk, dv, wq, wk, wv, n, deep=n > 0)
            by, guest = (*back, by)[0], [last.reshape(3, THIRD, -1)]
        size, *proj = settle(*guest, parts, devices, 0)
        return tuple(update(size, proj, feed, weights, m, v))

    states, all_of = P(("rep", "dp")), P()
    return jax.shard_map(
        step,
        mesh=mesh,
        in_specs=(states, states) + (all_of,) * 21,
        out_specs=(P("rep"),) * 21,
        check_vma=False,
    )
```

```python
import functools
import math

import jax
import jax.numpy as jnp
import numpy as np
from jax import lax
from jax.experimental import pallas as pl
from jax.experimental.pallas import tpu as pltpu
from jax.sharding import PartitionSpec as P

HEAD = 128
THETA = 10000
NAMES = ("wq", "wk", "wv", "wo", "w_gate", "w_up", "w_down")
NEG = -1e30
LOG2E = 1.4426950408889634
BF = jnp.bfloat16
F32 = jnp.float32
VMEM = 67_043_328
ROWS = 512
ANY = pl.BlockSpec(memory_space=pl.ANY)
ONE = pl.Buffered(1)


PART = 16
THIRD = PART * PART
THIRDS = range(3)
DMA = pltpu.SemaphoreType.DMA


def _ds(at, size, unit=PART):
    return pl.ds(pl.multiple_of(at, unit), size)


def _loop(count, body):
    lax.fori_loop(0, count, lambda n, _: body(n), None)


def _settle(copies):
    for c in copies:
        c.wait()


def _run(copies):
    for c in copies:
        c.start()


def _dot(ca, cb, a, b):
    return lax.dot_general(a, b, (((ca,), (cb,)), ((), ())), preferred_element_type=F32)


_nn, _nt, _tn = (functools.partial(_dot, *c) for c in ((1, 0), (1, 1), (0, 0)))


def _cols(n, size=HEAD):
    return slice(n * size, n * size + size)


def _zero(*refs):
    for ref in refs:
        ref[:] = jnp.zeros(ref.shape, F32)


def _bf(*shape):
    return jax.ShapeDtypeStruct(shape, BF)


def _f32(*shape):
    return jax.ShapeDtypeStruct(shape, F32)


def _params(**more):
    return pltpu.CompilerParams(vmem_limit_bytes=VMEM, **more)


def _norm(h):
    wide = h.astype(F32)
    scale = lax.rsqrt(jnp.mean(wide * wide, -1, keepdims=True) + 1e-6)
    return wide * scale, scale


def _norm_back(xhat, scale, by):
    return scale * (by - xhat * jnp.mean(xhat * by, -1, keepdims=True))


def _tables(tokens, rows):
    half = HEAD // 2
    freq = THETA ** (-np.arange(half) / half)
    freq, sign = np.concatenate([freq, freq]), np.concatenate([-np.ones(half), np.ones(half)])

    def of(places):
        angle = places[:, None] * freq
        return [np.asarray(x, np.float32) for x in (np.cos(angle), np.sin(angle) * sign)]

    return of(np.arange(0, tokens, rows)), of(np.arange(rows))


def _turns(i, refs):
    ca, sa = refs[0][pl.ds(i, 1), :], refs[1][pl.ds(i, 1), :]
    cb, sb = refs[2][:], refs[3][:]
    return ca * cb - sa * sb, sa * cb + ca * sb


def _turn(t, cos, sin):
    return (t * cos + pltpu.roll(t, HEAD // 2, 1) * sin).astype(BF)


def _turn_back(t, cos, sin):
    return (t * cos - pltpu.roll(t, HEAD // 2, 1) * sin).astype(BF)


def _rows(width, rows=ROWS):
    return pl.BlockSpec((rows, width), lambda i: (i, 0))


def _whole(a):
    return pl.BlockSpec(a.shape, lambda i: (0,) * a.ndim, pipeline_mode=ONE)


def _of_layer(w, number):
    return pl.BlockSpec((1, *w.shape[1:]), lambda i: (number, 0, 0), pipeline_mode=ONE)


def _attend(q_ref, k_s, v_s, o_ref, lse_ref, top_s, mix_s, row, group):
    bq, width = q_ref.shape
    heads = width // HEAD
    e = HEAD**-0.5 * LOG2E
    ones = jnp.ones((8, bq), BF)
    top_s[:] = jnp.full(top_s.shape, NEG, F32)
    _zero(mix_s)

    def block(j, masked):
        here = pl.ds(pl.multiple_of(j * bq, bq), bq)
        kept = _hidden(bq, bq) if masked else None
        scores = [_nt(k_s[here, _cols(n // group)], q_ref[:, _cols(n)]) for n in range(heads)]
        weights, keeps = [], []
        for n, s in enumerate(scores):
            if masked:
                s = jnp.where(kept, s, 2 * NEG)
            old = top_s[n : n + 1, :]
            top = jnp.maximum(old, s.max(axis=0, keepdims=True))
            top_s[n : n + 1, :] = top
            weights.append(jnp.exp2((s - top) * e).astype(BF))
            keeps.append(jnp.exp2((old - top) * e))
        values = [jnp.concatenate([v_s[here, _cols(g)].T, ones], axis=0) for g in range(heads // group)]
        for n, (p, keep) in enumerate(zip(weights, keeps)):
            mix_s[n] = mix_s[n] * keep + _nn(values[n // group], p)

    _loop(row, lambda j: block(j, False))
    block(row, True)
    for n in range(heads):
        total = mix_s[n, HEAD : HEAD + 1, :]
        o_ref[:, _cols(n)] = (mix_s[n, :HEAD, :] * (1 / total)).T.astype(BF)
        lse_ref[n : n + 1, :] = top_s[n : n + 1, :] * e + jnp.log2(total)


def _hidden(*shape):
    return lax.broadcasted_iota(jnp.int32, shape, 1) >= lax.broadcasted_iota(jnp.int32, shape, 0)


def _forward_kernel(x_ref, wq_ref, wk_ref, wv_ref, ca, sa, cb, sb, *refs, layers, blocks, group):
    take = iter(refs)
    some = lambda n: [next(take) for _ in range(n)]
    hbm = some(4)
    q_ref, k_ref, v_ref, o_ref, lse_ref, mid_ref, out_ref, bt_ref, *kept_hbm = some(10)
    k_s, v_s, h_s, top_s, mix_s, p_s, kept_s, load, sem, *weights = some(13)
    i = pl.program_id(0)
    row, layer = lax.rem(i, blocks), lax.div(i, blocks)
    here = _rows_at(row)
    loads = [pltpu.make_async_copy(ref.at[0], buf, load.at[n]) for n, (ref, buf) in enumerate(zip(hbm, weights))]
    tiles = kept_s.shape[1]

    def keeps(row):
        return [pltpu.make_async_copy(kept_s.at[w, n], ref.at[n, _rows_at(row), :], sem.at[w, n]) for n in range(tiles) for w, ref in enumerate(kept_hbm)]

    @pl.when(i == 0)
    def _():
        _run(loads)
        h_s[:] = jnp.zeros(h_s.shape, BF)

    cos, sin = _turns(row, (ca, sa, cb, sb))
    h = jnp.where(layer == 0, x_ref[:], h_s[here, :])
    a = _norm(h)[0].astype(BF)
    for w_ref, out in ((wq_ref, q_ref), (wk_ref, k_ref)):
        for at in range(w_ref.shape[2] // THIRD):
            t = _nn(a, w_ref[0, :, _cols(at, THIRD)]).astype(BF).astype(F32)
            for n in range(THIRD // HEAD):
                out[:, _cols(at * 2 + n)] = _turn(t[:, _cols(n)], cos, sin)
    v = _nn(a, wv_ref[0]).astype(BF)
    v_ref[:] = v
    v_s[here, :] = v
    k_s[here, :] = k_ref[:]
    _attend(q_ref, k_s, v_s, o_ref, lse_ref, top_s, mix_s, row, group)

    @pl.when(layer < layers - 1)
    def _():
        pl.when(i == 0)(lambda: _settle(loads))
        pl.when(i > 0)(lambda: _settle(keeps(row)))
        wo, wg, wu, wd = weights
        mid = jnp.where(layer == 0, x_ref[:], h_s[here, :]) + _nn(o_ref[:], wo[:]).astype(BF)
        mid_ref[:] = mid
        b = _norm(mid)[0].astype(BF)
        bt_ref[:] = b.T
        for n in range(tiles):
            gate, up = _nn(b, wg[:, _cols(n, THIRD)]), _nn(b, wu[:, _cols(n, THIRD)])
            kept_s[0, n] = gate
            kept_s[1, n] = up
            p_s[:, _cols(n, THIRD)] = (gate * jax.nn.sigmoid(gate) * up).astype(BF)
        _run(keeps(row))
        out = mid + _nn(p_s[:], wd[:]).astype(BF)
        out_ref[:] = out
        h_s[here, :] = out

    @pl.when(i == layers * blocks - 1)
    def _():
        _settle(keeps(row))


def _rows_at(row):
    return _ds(row * ROWS, ROWS)


def forward(x, weights):
    wq, wk, wv, *feed = weights
    layers, d, ff = feed[1].shape
    s = x.shape[0]
    blocks = s // ROWS
    tables = _tables(s, ROWS)
    nq, nk = wq.shape[2], wk.shape[2]
    row = lambda width: pl.BlockSpec((ROWS, width), lambda i: (i, 0))
    first = lambda i: jnp.minimum(i, blocks - 1)
    kept = pl.BlockSpec((ROWS, d), lambda i: (first(i), 0))
    of_layer = lambda w: pl.BlockSpec((1, *w.shape[1:]), lambda i: (lax.div(i, blocks), 0, 0))
    heads = nq // HEAD
    tile = _f32(ff // THIRD, s, THIRD)
    return pl.pallas_call(
        functools.partial(_forward_kernel, layers=layers, blocks=blocks, group=heads // (nk // HEAD)),
        grid=(layers * blocks,),
        in_specs=[kept, *(of_layer(w) for w in (wq, wk, wv)), *(_whole(t) for pair in tables for t in pair), *[ANY] * 4],
        out_specs=[row(nq), row(nk), row(nk), row(nq), pl.BlockSpec((8, ROWS), lambda i: (0, i)), kept, kept, pl.BlockSpec((d, ROWS), lambda i: (0, first(i))), ANY, ANY],
        out_shape=[*(_bf(layers * s, n) for n in (nq, nk, nk, nq)), _f32(8, layers * s), _bf(s, d), _bf(s, d), _bf(d, s), tile, tile],
        scratch_shapes=[*(pltpu.VMEM(shape, BF) for shape in ((s, nk), (s, nk), (s, d))), pltpu.VMEM((8, ROWS), F32), pltpu.VMEM((heads, HEAD + 8, ROWS), F32),
                        pltpu.VMEM((ROWS, ff), BF), pltpu.VMEM((2, ff // THIRD, ROWS, THIRD), F32), DMA((4,)), DMA((2, ff // THIRD)),
                        *(pltpu.VMEM(w.shape[1:], BF) for w in feed)],
        compiler_params=_params(),
        name="forward",
    )(x, wq, wk, wv, *(t for pair in tables for t in pair), *feed)


AXES = ((8, 4, 2), (4, 2, 8), (2, 8, 4))
CORE = 1
HALF = THIRD // 2
QUARTER = HALF // 2
EIGHTH = QUARTER // 2
NEAR = (CORE, *AXES[0])
MESH = pl.DeviceIdType.MESH
SIDES = 4


def _bit(stride):
    return lax.rem(lax.div(lax.axis_index("dp"), stride), 2)


def _peer(stride):
    return {"dp": lax.axis_index("dp") + stride * (1 - 2 * _bit(stride))}


def _greet(peers):
    barrier = pltpu.get_barrier_semaphore()
    for peer in peers:
        pl.semaphore_signal(barrier, device_id=peer, device_id_type=MESH)
    pl.semaphore_wait(barrier, len(peers))


def _send(src, dst, sems, at, peer):
    return pltpu.make_async_remote_copy(src, dst, sems[0].at[at], sems[1].at[at], device_id=peer, device_id_type=MESH)


class Scatter:
    def __init__(self, mine, dst, bufs, sems):
        self.mine, self.dst, self.sems = mine, dst, sems
        self.r0, *self.got, self.sum = bufs

    @staticmethod
    def scratch(width, slots):
        rows = (HALF, QUARTER, EIGHTH, PART, HALF)
        return [pltpu.VMEM((slots, 3, n, width), BF) for n in (THIRD, *rows)] + [DMA((slots, 3, 5))] * 2

    @staticmethod
    def of(scratch, n, dst):
        mine, *bufs, sent, got = [ref.at[lax.rem(n, ref.shape[0])] for ref in scratch]
        return Scatter(mine, dst, bufs, (sent, got))

    def _core(self, t, late):
        b = _bit(AXES[t][0])
        at = QUARTER * (b if late else 1 - b)
        return _send(self.mine.at[t, _ds(HALF * (1 - _bit(CORE)) + at, QUARTER), :], self.r0.at[t, _ds(at, QUARTER), :], self.sems, (t, 3 + late), _peer(CORE))

    def _over(self, t, k):
        size = QUARTER >> k
        return _send(self.sum.at[t, HALF - 2 * size : HALF - size, :], self.got[k].at[t], self.sems, (t, k), _peer(AXES[t][k]))

    def start(self):
        for late in (False, True):
            for t in THIRDS:
                self._core(t, late).start()

    def _add(self, t, k, dst):
        bits = [_bit(stride) for stride in AXES[t]]
        if k < 3:
            bits[k] = 1 - bits[k]
        size = QUARTER >> min(k, 2)
        at = [sum(b * (QUARTER >> n) for n, b in list(enumerate(bits[: k + 1]))[m:]) for m in range(min(k, 2) + 2)]
        total = self.mine[t, _ds(HALF * _bit(CORE) + at[0], size), :].astype(F32) + self.r0[t, _ds(at[0], size), :].astype(F32)
        for n in range(k):
            total += self.got[n][t, _ds(at[n + 1] if n < 2 else 0, size), :].astype(F32)
        dst[:] = total.astype(BF)

    def halve(self, k):
        for t in THIRDS:
            if k < 2:
                self._core(t, bool(k)).wait()
            if k:
                self._over(t, k - 1).wait()
        size = QUARTER >> k
        for t in THIRDS:
            self._add(t, k, self.sum.at[t, HALF - 2 * size : HALF - size, :])
        for t in THIRDS:
            self._over(t, k).start()

    def finish(self):
        for t in THIRDS:
            self._over(t, 2).wait()
        for t in THIRDS:
            self._add(t, 3, self.dst.at[t])


class Gather:
    def __init__(self, own, everything, sems):
        self.own, self.all, self.sems = own, everything, sems

    @staticmethod
    def scratch(own):
        return [pltpu.VMEM(own.shape, BF), DMA((4,)), DMA((3, 9)), DMA((3, 9))]

    def _move(self, t, k, axis=True):
        bits = [_bit(CORE), *(_bit(stride) for stride in AXES[t])]
        over = THIRDS[-1 - min(max(k, 0), 2)]
        if k == 3:
            bits[2] = 1 - bits[2]
        if k >= 0 and not axis:
            bits[1 + over] = 1 - bits[1 + over]
        count = 1 << min(max(k, 0), 1)
        there = self.all.at[t, pl.ds(sum(b * (8 >> n) for n, b in enumerate(bits) if 8 >> n >= count), count)]
        src = there if k > 0 or not axis and k == 0 else self.own.at[pl.ds(t, 1)]
        return _send(src, there, self.sems, (t, k if axis else 5 + k), _peer(AXES[t][over] if axis else CORE))

    def place(self, sem):
        return [pltpu.make_async_copy(self.own.at[pl.ds(t, 1)], self._move(t, -1, False).dst_ref, sem.at[t]) for t in THIRDS]

    def start(self):
        for t in THIRDS:
            self._move(t, 0).start()
            self._move(t, -1, False).start()

    def double(self, k):
        for t in THIRDS:
            self._move(t, k).wait_recv()
            if k == 0:
                self._move(t, 1).start()
            elif k == 1:
                self._move(t, 3).start()
            self._move(t, k, False).start()
        if k == 0:
            for t in THIRDS:
                self._move(t, 2).start()

    def finish(self):
        for t in THIRDS:
            for k in range(4):
                self._move(t, k).wait_send()
                self._move(t, k, False).wait()
            self._move(t, -1, False).wait()


class Gathers:
    def __init__(self, own, everything, scratch):
        self.units = []
        for n, (o, a) in enumerate(zip(own, everything)):
            stage, sem, *sems = scratch[4 * n : 4 * n + 4]
            self.units.append((Gather(stage, a, sems), pltpu.make_async_copy(o, stage, sem.at[3]), sem))

    def load(self):
        _run([load for _, load, _ in self.units])

    def start(self):
        for g, load, sem in self.units:
            load.wait()
            g.start()
            _run(g.place(sem))

    def double(self, k):
        for g, _, sem in self.units:
            if k == 0:
                _settle(g.place(sem))
            g.double(k)

    def finish(self):
        for g, *_ in self.units:
            g.finish()

    @staticmethod
    def outs(parts):
        return [_bf(3, PART, *p.shape[1:]) for p in parts]

    @staticmethod
    def scratch(parts):
        return [s for p in parts for s in Gather.scratch(p)]


def _feed_back_kernel(*refs, fresh, number, tiles, guest):
    take = iter(refs)
    some = lambda n: [next(take) for _ in range(n)]
    o_hbm, mid_hbm, dy_hbm, wo_hbm, wg_hbm, wu_hbm, wd_hbm = some(7)
    kept = [] if fresh else some(3)
    guests = some(min(guest, 1))
    by_hbm, do_hbm, delta_ref, own_ref = some(4)
    guest_all = some(min(guest, 1))
    dy_s, wo_s, wg_s, wu_s, dg_s, du_s, load, pair_sem = some(8)
    room = some(8)
    gathers = [(Gather(own_ref.at[:, :guest], ref, some(2)), some(1)[0]) for ref in guest_all]
    tile_s = room[0]
    slots = tile_s.shape[0]
    s, d = dy_s.shape
    width = THIRD
    blocks = s // ROWS
    rows = _rows_at
    halves = [functools.partial(Scatter.halve, k=k) for k in THIRDS]

    run, settle = _run, _settle

    def tell(now, acts):
        for act, back, first, last in acts:
            n = now - back

            @pl.when((n >= first) & (n <= last))
            def _():
                act(Scatter.of(room, n + 2 * guest, own_ref.at[:, n + guest]))

    def acts(last):
        backs = (Scatter.finish, slots), (halves[2], slots - 1), (halves[1], slots - 2), (halves[0], 2), (Scatter.start, 1)
        return [(act, back, -guest, last if back > 2 else tiles - 1) for act, back in backs]

    def row_loads(r, bufs):
        here = rows(r) if fresh else slice(None)
        there = _rows_at(number * blocks + r), rows(r)
        return [pltpu.make_async_copy(hbm.at[at, :], buf.at[here, :], pair_sem.at[n]) for n, (hbm, at, buf) in enumerate(zip((o_hbm, mid_hbm), there, bufs))]

    late_loads = [pltpu.make_async_copy(hbm.at[number], buf, load.at[n]) for n, (hbm, buf) in enumerate(((wo_hbm, wo_s), (wg_hbm, wg_s), (wu_hbm, wu_s)))]

    def tile_phase(wd_s, wd_sem, bt_s, p_s, *more):
        pairs = [(dy_hbm, dy_s)] if fresh else [(dy_hbm, dy_s), (kept[2], bt_s.at[:, :s])]
        pairs += [(ref.at[n], tile_s.at[(n + guest) % slots]) for ref in guests for n in range(guest)]
        loads = [pltpu.make_async_copy(*pair, load.at[3 + n]) for n, pair in enumerate(pairs)]

        def down(n):
            slot = lax.rem(n, 2)
            return pltpu.make_async_copy(wd_hbm.at[number, _ds(lax.rem(n, tiles) * width, width), :], wd_s.at[slot], wd_sem.at[slot])

        def fetch(n):
            slot = lax.rem(n, 2)
            return [pltpu.make_async_copy(ref.at[lax.rem(n, tiles)], more[0].at[slot, w], more[1].at[slot, w]) for w, ref in enumerate(kept[:2])]

        run([down(0)] + (row_loads(0, more[1:]) + late_loads + loads if fresh else loads[::-1] + fetch(0)))
        _greet([_peer(stride) for stride in NEAR])
        settle(loads[2:])
        _loop(max(guest - 1, 0), lambda n: tell(n + 1 - guest, acts(0)))
        if fresh:
            b_s, *bufs = more
            o_s, mid_s = bufs
            settle(late_loads[:1])

            def prepare(r):
                settle(row_loads(r, bufs))
                pl.when(r + 1 < blocks)(lambda: run(row_loads(r + 1, bufs)))
                mid = mid_s[rows(r), :] + _nn(o_s[rows(r), :], wo_s[:]).astype(BF)
                mid_s[rows(r), :] = mid
                b = _norm(mid)[0].astype(BF)
                b_s[rows(r), :] = b
                bt_s[:, _ds(r * ROWS, ROWS, ROWS)] = b.T

            _loop(blocks, prepare)
            settle(late_loads[1:] + loads)
        else:
            settle(loads[:2])
            run(late_loads)

        def tile(i):
            tell(i, acts(tiles))
            pl.when(i == tiles - 1)(begin)
            f = _ds(i * width, width, width)
            settle([down(i)] + fetch(i))
            run([down(i + 1)] + fetch(i + 1))
            wd = wd_s[lax.rem(i, 2)]
            for r in range(blocks):
                here = _cols(r, ROWS)
                if fresh:
                    gate, up = _nn(b_s[here, :], wg_s[:, f]), _nn(b_s[here, :], wu_s[:, f])
                else:
                    gate, up = (more[0][lax.rem(i, 2), w, here, :] for w in range(2))
                dp = _nt(dy_s[here, :], wd).astype(BF).astype(F32)
                sig = jax.nn.sigmoid(gate)
                silu = gate * sig
                p_s[here, :] = (silu * up).astype(BF)
                du_s[here, f] = (dp * silu).astype(BF)
                dg_s[here, f] = (dp * up * (sig * (1 + gate * (1 - sig)))).astype(BF)
            new = tile_s.at[lax.rem(i + 2 * guest, slots)]
            for n, right in enumerate((dg_s[:, f], du_s[:, f])):
                out = _nn(bt_s[:, :s], right).astype(BF)
                for t in THIRDS:
                    new[t, :, _cols(n, width)] = out[_cols(t, THIRD), :]
            out = _tn(p_s[:], dy_s[:]).astype(BF)
            for t in THIRDS:
                new[t, :, 2 * width :] = out[:, _cols(t, width)]

        _loop(tiles, tile)
        settle([down(tiles)] + fetch(tiles))

    def begin():
        for gather, sem in gathers:
            gather.start()
            _run(gather.place(sem))

    def row_phase(by_s, do_s, sem, *bufs):
        def row_stores(r):
            return [pltpu.make_async_copy(buf, hbm.at[rows(r), :], sem.at[n]) for n, (hbm, buf) in enumerate(((by_hbm, by_s), (do_hbm, do_s)))]

        if not fresh:
            settle(late_loads)

        def row(r):
            tell(tiles + r, acts(tiles - 2) + [(halves[1 + n], slots - 3 + n, tiles - 1, tiles - 1) for n in (1, 0)])
            for gather, sem in gathers:
                pl.when(r == 0)(lambda: _settle(gather.place(sem)))
                for k in range(blocks):
                    pl.when(r == k)(functools.partial(gather.double, k))
            here = rows(r)
            part = here if fresh else slice(None)
            if not fresh:
                run(row_loads(r, bufs))
            db = (_nt(dg_s[here, :], wg_s[:]) + _nt(du_s[here, :], wu_s[:])).astype(BF).astype(F32)
            if not fresh:
                settle(row_loads(r, bufs))
            pl.when(r > 0)(lambda: settle(row_stores(r - 1)))
            o_s, mid_s = bufs
            xhat, scale = _norm(mid_s[part, :])
            by = dy_s[here, :] + _norm_back(xhat, scale, db).astype(BF)
            by_s[:] = by
            do = _nt(by, wo_s[:]).astype(BF)
            do_s[:] = do
            run(row_stores(r))
            both = do.astype(F32) * o_s[part, :].astype(F32)
            for n in range(d // HEAD):
                delta_ref[n : n + 1, _ds(r * ROWS, ROWS, ROWS)] = both[:, _cols(n)].T.sum(axis=0, keepdims=True)

        _loop(blocks, row)
        settle(row_stores(blocks - 1))

    vmem = lambda *shape: pltpu.VMEM(shape, BF)
    kinds = [vmem(2, width, d), DMA((2,)), vmem(d, s + HEAD), vmem(s, width)]
    out = [vmem(ROWS, d), vmem(ROWS, d)]
    if fresh:

        def all_phases(*bufs):
            pl.run_scoped(lambda *a: tile_phase(*a, *bufs), *kinds, vmem(s, d))
            pl.run_scoped(lambda *a: row_phase(*a, *bufs), *out, DMA((2,)))

        pl.run_scoped(all_phases, vmem(s, d), vmem(s, d))
    else:
        pl.run_scoped(tile_phase, *kinds, pltpu.VMEM((2, 2, s, width), F32), DMA((2, 2)))
        pl.run_scoped(row_phase, *out, DMA((2,)), *out)
    for n in (tiles - 2, tiles - 1):
        Scatter.of(room, n + 2 * guest, own_ref.at[:, n + guest]).finish()
    for gather, _ in gathers:
        gather.finish()


def feed_back(o, h, dy, weights, number, collective_id, kept=(), guest=(), slots=6):
    s, d = h.shape
    ff = weights[1].shape[2]
    tiles = ff // THIRD
    fresh = not kept
    tiles_in = guest[0].shape[0] if guest else 0
    own = _bf(3, tiles_in + tiles, PART, d)
    scratch = [pltpu.VMEM(shape, BF) for shape in ((s, d), *(w.shape[1:] for w in weights[:3]), (s, ff), (s, ff))]
    in_vmem = pl.BlockSpec(memory_space=pltpu.VMEM)
    return pl.pallas_call(
        functools.partial(_feed_back_kernel, fresh=fresh, number=number, tiles=tiles, guest=tiles_in),
        in_specs=[ANY] * (7 + len(kept) + len(guest)),
        out_specs=[ANY, ANY, in_vmem, in_vmem, *[ANY] * len(guest)],
        out_shape=[_bf(s, d), _bf(s, d), _f32(8, s), own, *(_bf(3, PART, tiles_in, PART, d) for _ in guest)],
        scratch_shapes=[*scratch, DMA((8,)), DMA((2,)), *Scatter.scratch(d, slots), *[DMA((3, 9)), DMA((3, 9)), DMA((3,))] * len(guest)],
        compiler_params=_params(collective_id=collective_id, has_side_effects=True),
        name="feed_back",
    )(o, h, dy, *weights, *kept, *guest)


def _attend_back_kernel(q_ref, k_ref, v_ref, do_ref, lse_ref, delta_ref, *rest, bk, group, units, first):
    own, rest = rest[:units], rest[units:]
    dq_ref, dk_ref, dv_ref, *rest = rest
    everything, rest = rest[:units], rest[units:]
    dq_s, dk_s, dv_s, *rest = rest
    work = Gathers([ref.at[:, first:] for ref in own], everything, rest)
    bq, width = q_ref.shape
    heads = width // HEAD
    iq = pl.program_id(0)
    last = pl.num_programs(0) - 1
    scale = HEAD**-0.5
    e = scale * LOG2E

    @pl.when(iq == 0)
    def _():
        work.load()
        _greet([_peer(stride) for stride in NEAR])
        work.start()
        _zero(dk_s, dv_s)

    _zero(dq_s)

    def block(j, first):
        here = _ds(j * bk, bk)
        at = first or 0
        kept = None if first is None else _hidden(bk, bq - at)
        scores, dps = [], []
        for n in range(heads):
            g = n // group
            scores.append(_nt(k_ref[here, _cols(g)], q_ref[at:, _cols(n)]))
            dps.append(_nt(v_ref[here, _cols(g)], do_ref[at:, _cols(n)]))
        for n in range(heads):
            g = n // group
            p = jnp.exp2(scores[n] * e - lse_ref[n : n + 1, at:])
            if first is not None:
                p = jnp.where(kept, p, 0.0)
            ds = (p * (dps[n] - delta_ref[n : n + 1, at:])).astype(BF)
            dv_s[g, here, :] += _nn(p.astype(BF), do_ref[at:, _cols(n)])
            dk_s[g, here, :] += _nn(ds, q_ref[at:, _cols(n)])
            dq_s[n, :, at:] += _nn(k_ref[here, _cols(g)].T, ds)

    per = bq // bk
    _loop(iq * per, lambda j: block(j, None))
    for n in THIRDS:
        pl.when(iq == last - 2 + n)(functools.partial(work.double, n))
    for n in range(per):
        block(iq * per + n, n * bk)
    pl.when(iq == last)(lambda: work.double(3))
    for n in range(heads):
        dq_ref[:, _cols(n)] = (dq_s[n] * scale).T.astype(BF)

    @pl.when(iq == last)
    def _():
        for g in range(heads // group):
            dk_ref[:, _cols(g)] = (dk_s[g] * scale).astype(BF)
            dv_ref[:, _cols(g)] = dv_s[g].astype(BF)
        work.finish()


def attend_back(q, k, v, do, lse, delta, parts, first, number, collective_id, bq=ROWS, bk=THIRD):
    s, width = do.shape
    heads, groups = width // HEAD, k.shape[1] // HEAD
    base = number * (s // bq)
    mine = lambda a: pl.BlockSpec((s, a.shape[1]), lambda i: (number, 0), pipeline_mode=ONE)
    out = [_bf(s, t.shape[1]) for t in (q, k, v)]
    mine_own = [_bf(3, p.shape[1] - first, *p.shape[2:]) for p in parts]
    return pl.pallas_call(
        functools.partial(_attend_back_kernel, bk=bk, group=heads // groups, units=len(parts), first=first),
        grid=(s // bq,),
        in_specs=[pl.BlockSpec((bq, width), lambda i: (base + i, 0)), mine(k), mine(v), _rows(width, bq), pl.BlockSpec((8, bq), lambda i: (0, base + i)),
                  pl.BlockSpec((8, bq), lambda i: (0, i)), *[ANY] * len(mine_own)],
        out_specs=[_rows(width, bq), *(_whole(t) for t in out[1:]), *[ANY] * len(mine_own)],
        out_shape=[*out, *Gathers.outs(mine_own)],
        scratch_shapes=[pltpu.VMEM(shape, F32) for shape in ((heads, HEAD, bq), (groups, s, HEAD), (groups, s, HEAD))] + Gathers.scratch(mine_own),
        compiler_params=_params(collective_id=collective_id, has_side_effects=True),
        name="attend_back",
    )(q, k, v, do, lse, delta, *parts)


def _squares(ref, total):
    tiles = ref.shape[1]

    def one(n, total):
        g = ref[lax.div(n, tiles), lax.rem(n, tiles)].astype(F32)
        return total + g * g

    return lax.fori_loop(0, len(THIRDS) * tiles, one, total)


Q, KV, OUT = THIRDS


def _proj_back_kernel(*refs, parts, devices, number):
    take = iter(refs)
    some = lambda n: [next(take) for _ in range(n)]
    h_hbm, by_hbm, o_hbm, dq_hbm, dk_hbm, dv_hbm, *tables = some(10)
    deep = parts == 0
    if deep:
        w_hbm = some(3)
        out_hbm, g_hbm = some(2)
    else:
        parts = some(parts)
        size_ref, all_ref = some(2)
    h_s, by_s, o_s, t_s, at_s, load, tile_s = some(7)
    s, d = h_s.shape
    nq, nk = dq_hbm.shape[1], dk_hbm.shape[1]
    blocks = s // ROWS
    spots = [slice(0, nq), slice(nq, nq + nk), slice(nq + nk, nq + 2 * nk)]
    pairs = [(o_hbm.at[_ds(number * s, s), :], o_s), (by_hbm, by_s), (h_hbm, h_s), *((ref, t_s.at[:, at]) for ref, at in zip((dq_hbm, dk_hbm, dv_hbm), spots))]
    loads = [pltpu.make_async_copy(*pair, load.at[n]) for n, pair in enumerate(pairs)]
    _run(loads)
    if deep:
        w_s, out_s, sems = some(3)
        weights = [pltpu.make_async_copy(ref.at[number], w_s.at[:, at], sems.at[n]) for n, (ref, at) in enumerate(zip(w_hbm, spots))]
        _run(weights)
    else:
        room = [tile_s, *some(7)]
        own_s, local, slots, *sems = some(9)
        tiles = own_s.shape[1]
        work = [Scatter.of(room, n, own_s.at[:, n]) for n in range(tiles)]
        gathers = [Gather(own_s.at[:, at], all_ref.at[:, :, at], pair) for at, pair in ((slice(OUT), sems[:OUT]), (slice(OUT, tiles), sems[OUT:SIDES]))]
        places = [g.place(local.at[n]) for n, g in enumerate(gathers)]
        me = lax.axis_index("dp")
        others = [lax.rem(me + n, devices) for n in range(1, devices)]
        _greet([{"dp": other} for other in others])

    def put(n, value):
        for t in THIRDS:
            tile_s[n, t, :, : value.shape[1]] = value[_cols(t, THIRD), :].astype(BF)

    _settle(loads[:2])
    put(OUT, _tn(o_s[:], by_s[:]))
    if not deep:
        work[OUT].start()
    _settle(loads[2:])

    def prepare(r):
        here = _ds(r * ROWS, ROWS)
        cos, sin = _turns(r, tables)
        for n in range((nq + nk) // HEAD):
            t_s[here, _cols(n)] = _turn_back(t_s[here, _cols(n)].astype(F32), cos, sin)
        at_s[:, _ds(r * ROWS, ROWS, ROWS)] = _norm(h_s[here, :])[0].astype(BF).T

    _loop(blocks, prepare)
    if not deep:
        work[OUT].halve(Q)
    put(Q, _nn(at_s[:, :s], t_s[:, :nq]))
    if not deep:
        work[Q].start()
        work[OUT].halve(KV)
    put(KV, jnp.zeros((d, d), BF))
    put(KV, _nn(at_s[:, :s], t_s[:, nq:]))
    if deep:
        g_copy = pltpu.make_async_copy(tile_s, g_hbm, load.at[0])
        g_copy.start()
        _settle(weights)

        def store(r):
            return pltpu.make_async_copy(out_s.at[lax.rem(r, 2)], out_hbm.at[_ds(r * ROWS, ROWS), :], sems.at[lax.rem(r, 2)])

        def row(r):
            here = _ds(r * ROWS, ROWS)
            da = _nt(t_s[here, :], w_s[:]).astype(BF).astype(F32)
            xhat, scale = _norm(h_s[here, :])
            pl.when(r > 1)(lambda: store(r - 2).wait())
            out_s[lax.rem(r, 2)] = by_s[here, :] + _norm_back(xhat, scale, da).astype(BF)
            store(r).start()

        _loop(blocks, row)
        g_copy.wait()
        _settle([store(blocks - 2), store(blocks - 1)])
        return
    work[KV].start()
    work[OUT].halve(OUT)
    work[Q].halve(Q)
    total = jnp.zeros((PART, d), F32)
    for ref in parts:
        total = _squares(ref, total)
    work[KV].halve(Q)
    work[OUT].finish()

    def begin(n):
        gathers[n].start()
        _run(places[n])

    def double(n, k):
        if k == Q:
            _settle(places[n])
        gathers[n].double(k)

    begin(KV)
    for k in (KV, OUT):
        for n in (Q, KV):
            work[n].halve(k)
    double(KV, Q)
    for n in (Q, KV):
        work[n].finish()
    begin(Q)
    slots[me] = jnp.full(size_ref.shape, jnp.sum(_squares(own_s, total)), F32)
    copies = [_send(slots.at[me], slots.at[me], sems[SIDES:], n, {"dp": other}) for n, other in enumerate(others)]
    _run(copies)
    double(KV, KV)
    double(Q, Q)
    double(KV, OUT)
    _settle(copies)
    size_ref[:] = sum(slots[n] for n in range(devices))
    double(KV, len(THIRDS))
    for k in range(KV, SIDES):
        double(Q, k)
    for g in gathers:
        g.finish()


def proj_back(h, by, o, dq, dk, dv, weights=(), number=0, parts=(), devices=0, collective_id=0):
    s, d = h.shape
    (ca, sa), (cb, sb) = _tables(s, ROWS)
    wide = dq.shape[1] + 2 * dk.shape[1]
    vmem = lambda *shape: pltpu.VMEM(shape, BF)
    in_vmem = pl.BlockSpec(memory_space=pltpu.VMEM)
    scratch = [*[vmem(s, d)] * 3, vmem(s, wide), vmem(d, s + HEAD), DMA((6,))]
    own = _bf(3, 3, PART, d)
    if weights:
        scratch += [vmem(3, 3, THIRD, d), vmem(d, wide), vmem(2, ROWS, d), DMA((3,))]
        outs = [ANY] * 2, [_bf(s, d), _bf(3, 3, THIRD, d)]
    else:
        scratch += Scatter.scratch(d, 3) + [vmem(*own.shape), DMA((2, 3)), pltpu.VMEM((devices, 8, HEAD), F32), *[DMA((3, 9))] * SIDES, *[DMA((devices,))] * 2]
        outs = [in_vmem, ANY], [_f32(8, HEAD), *Gathers.outs([own])]
    return pl.pallas_call(
        functools.partial(_proj_back_kernel, parts=len(parts), devices=devices, number=number),
        in_specs=[*[ANY] * 6, *[in_vmem] * 4, *[ANY] * len(weights), *[in_vmem] * len(parts)],
        out_specs=outs[0],
        out_shape=outs[1],
        scratch_shapes=scratch,
        compiler_params=_params() if weights else _params(collective_id=collective_id, has_side_effects=True),
        name="proj_back",
    )(h, by, o, dq, dk, dv, ca, sa, cb, sb, *weights, *parts)


KINDS = (BF, F32, F32) * 2
NEW = range(3, len(KINDS))


def _update_kernel(size_ref, *refs, layers, slots, count):
    take = iter(refs)
    some = lambda n: [next(take) for _ in range(n)]
    proj, feed = some(layers), some(layers)
    hbm = [some(len(NAMES)) for _ in KINDS]
    flat, deep = some(len(KINDS)), some(len(KINDS))
    gp_s, gf_s, in_sem, g_sem, out_sem = take
    rows = flat[0].shape[1]
    sixteenths = rows // PART
    tiles = gf_s.shape[2]
    steps = 3 * PART // sixteenths
    factor = jnp.minimum(1.0, 0.5 * lax.rsqrt(size_ref[0:1, 0:1] / count + 1e-30))
    narrow = flat[0].shape[2] - 2 * tiles * THIRD

    def moves(k, layer, i, slot):
        sem = out_sem.at[slot, k % 3] if k in NEW else in_sem.at[slot, k]
        at = 0
        for ref in hbm[k][:6]:
            there, here = ref.at[layer, _ds(i * rows, rows), :], flat[k].at[slot, :, at : at + ref.shape[2]]
            yield pltpu.make_async_copy(here, there, sem) if k in NEW else pltpu.make_async_copy(there, here, sem)
            at += ref.shape[2]
        per = PART // sixteenths
        there = hbm[k][6].at[layer, :, _ds(lax.rem(i, per) * rows, rows), _ds(lax.div(i, per) * THIRD, THIRD, THIRD)]
        yield pltpu.make_async_copy(deep[k].at[slot], there, sem) if k in NEW else pltpu.make_async_copy(there, deep[k].at[slot], sem)

    def fetch(layer, i, slot):
        per = PART // sixteenths
        for n, (ref, buf) in enumerate(((proj[layer], gp_s), (feed[layer], gf_s))):
            pltpu.make_async_copy(ref.at[lax.div(i, per), pl.ds(lax.rem(i, per) * sixteenths, sixteenths)], buf.at[slot], g_sem.at[slot, n]).start()
        for k in THIRDS:
            for c in moves(k, layer, i, slot):
                c.start()

    def settled(k, slot):
        sem = out_sem.at[slot, k % 3] if k in NEW else in_sem.at[slot, k]
        for buf in (flat[k], deep[k]):
            pltpu.make_async_copy(buf.at[slot], buf.at[slot], sem).wait()

    def advance(g, bufs, at):
        g = g.astype(F32) * factor
        w, m, v = (buf[at].astype(F32) for buf in bufs[:3])
        m = 0.9 * m + 0.1 * g
        v = 0.95 * v + 0.05 * g * g
        for buf, new in zip(bufs[3:], (w - 0.02 * (m * lax.rsqrt(v + 1e-8) + 0.1 * w), m, v)):
            buf[at] = new.astype(buf.dtype)

    def one(layer):
        def step(i):
            n = layer * steps + i
            slot = lax.rem(n, slots)

            @pl.when(n >= slots)
            def _():
                for k in NEW:
                    settled(k, slot)

            for n, buf in enumerate((gp_s, gf_s)):
                pltpu.make_async_copy(buf.at[slot], buf.at[slot], g_sem.at[slot, n]).wait()
            for k in THIRDS:
                settled(k, slot)

            def tile(f):
                for n in range(sixteenths):
                    here = _cols(n, PART)
                    for w in range(2):
                        advance(gf_s[slot, n, f, :, _cols(w, THIRD)], flat, (slot, here, _ds(narrow + (w * tiles + f) * THIRD, THIRD, THIRD)))
                    advance(gf_s[slot, n, f, :, 2 * THIRD :], deep, (slot, f, here))

            _loop(tiles, tile)

            def plain(f):
                for n in range(sixteenths):
                    across = _ds(f * THIRD, THIRD, THIRD)
                    place = jnp.where(f < 5, f, f + 1)
                    g = gp_s[slot, n, lax.div(place, 3), :, _ds(lax.rem(place, 3) * THIRD, THIRD, THIRD)]
                    advance(g, flat, (slot, _cols(n, PART), across))

            _loop(narrow // THIRD, plain)
            for k in NEW:
                for c in moves(k, layer, i, slot):
                    c.start()
            ahead = i + slots
            pl.when(ahead < steps)(lambda: fetch(layer, ahead, slot))
            if layer + 1 < layers:
                pl.when(ahead >= steps)(lambda: fetch(layer + 1, ahead - steps, slot))

        _loop(steps, step)

    for slot in range(slots):
        fetch(0, slot, slot)
    for layer in range(layers):
        one(layer)
    for slot in range(slots):
        for k in NEW:
            settled(k, slot)


def update(size, proj, feed, weights, m, v, slots=3, sixteenths=2):
    layers, d, ff = weights[4].shape
    rows = sixteenths * PART
    split = lambda a: a.reshape(layers, -1, THIRD, d)
    state = [a for kind in (weights, m, v) for a in (*kind[:6], split(kind[6]))]
    flat = [pltpu.VMEM((slots, rows, sum(w.shape[2] for w in weights[:6])), kind) for kind in KINDS]
    deep = [pltpu.VMEM((slots, ff // THIRD, rows, THIRD), kind) for kind in KINDS]
    grads = [pltpu.VMEM((slots, sixteenths, *g.shape[2:]), BF) for g in (proj[0], feed[0])]
    count = sum(w.size for w in weights)
    new = pl.pallas_call(
        functools.partial(_update_kernel, layers=layers, slots=slots, count=count),
        in_specs=[pl.BlockSpec(memory_space=pltpu.VMEM), *[ANY] * (2 * layers + 21)],
        out_specs=[ANY] * 21,
        out_shape=[jax.ShapeDtypeStruct(a.shape, a.dtype) for a in state],
        scratch_shapes=[*flat, *deep, *grads, DMA((slots, 3)), DMA((slots, 2)), DMA((slots, 3))],
        compiler_params=_params(),
        name="update",
    )(size, *proj, *feed, *state)
    return [a.reshape(old.shape) for a, old in zip(new, (*weights, *m, *v))]


def solution(mesh):
    devices = mesh.shape["dp"]

    def step(x, dy, *arrays):
        weights, m, v = (arrays[i : i + 7] for i in (0, 7, 14))
        wq, wk, wv, *feeds = weights
        layers = wq.shape[0]
        q, k, v_, o, lse, mid, out, *kept = forward(x[0], weights)
        by, guest = dy[0], ()
        parts, proj, feed = [], [], [None] * layers
        for n in reversed(range(layers)):
            last = n == layers - 1
            h = out if n else x[0]
            by, do, delta, own, *more = feed_back(o, h if last else mid, by, feeds, n, 2 * n + 1, () if last else (kept[1], kept[2], kept[0]), guest)
            proj += more
            dq, dk, dv, feed[n] = attend_back(q, k, v_, do, lse, delta, [own], 0 if last else wq.shape[1] // THIRD, n, 2 * n + 2)
            parts.append(own)
            if n:
                by, *guest = proj_back(h, by, o, dq, dk, dv, (wq, wk, wv), n)
        size, *first = proj_back(h, by, o, dq, dk, dv, parts=parts, devices=devices)
        return tuple(update(size, first + proj, feed, weights, m, v))

    states, all_of = P(("rep", "dp")), P()
    return jax.shard_map(
        step,
        mesh=mesh,
        in_specs=(states, states) + (all_of,) * 21,
        out_specs=(P("rep"),) * 21,
        check_vma=False,
    )
```

```python
import functools
import math

import jax
import jax.numpy as jnp
import numpy as np
from jax import lax
from jax.experimental import pallas as pl
from jax.experimental.pallas import tpu as pltpu
from jax.sharding import PartitionSpec as P

HEAD = 128
THETA = 10000
NAMES = ("wq", "wk", "wv", "wo", "w_gate", "w_up", "w_down")
NEG = -1e30
LOG2E = 1.4426950408889634
BF = jnp.bfloat16
F32 = jnp.float32
VMEM = 67_043_328
ROWS = 512
ANY = pl.BlockSpec(memory_space=pl.ANY)
ONE = pl.Buffered(1)


PART = 16
THIRD = PART * PART
THIRDS = range(3)
DMA = pltpu.SemaphoreType.DMA


def _ds(at, size, unit=PART):
    return pl.ds(pl.multiple_of(at, unit), size)


def _loop(count, body):
    lax.fori_loop(0, count, lambda n, _: body(n), None)


def _settle(copies):
    for c in copies:
        c.wait()


def _run(copies):
    for c in copies:
        c.start()


def _dot(ca, cb, a, b):
    return lax.dot_general(a, b, (((ca,), (cb,)), ((), ())), preferred_element_type=F32)


_nn, _nt, _tn = (functools.partial(_dot, *c) for c in ((1, 0), (1, 1), (0, 0)))


def _cols(n, size=HEAD):
    return slice(n * size, n * size + size)


def _zero(*refs):
    for ref in refs:
        ref[:] = jnp.zeros(ref.shape, F32)


def _bf(*shape):
    return jax.ShapeDtypeStruct(shape, BF)


def _f32(*shape):
    return jax.ShapeDtypeStruct(shape, F32)


def _params(**more):
    return pltpu.CompilerParams(vmem_limit_bytes=VMEM, **more)


def _norm(h):
    wide = h.astype(F32)
    scale = lax.rsqrt(jnp.mean(wide * wide, -1, keepdims=True) + 1e-6)
    return wide * scale, scale


def _norm_back(xhat, scale, by):
    return scale * (by - xhat * jnp.mean(xhat * by, -1, keepdims=True))


def _tables(tokens, rows):
    half = HEAD // 2
    freq = THETA ** (-np.arange(half) / half)
    freq, sign = np.concatenate([freq, freq]), np.concatenate([-np.ones(half), np.ones(half)])

    def of(places):
        angle = places[:, None] * freq
        return [np.asarray(x, np.float32) for x in (np.cos(angle), np.sin(angle) * sign)]

    return of(np.arange(0, tokens, rows)), of(np.arange(rows))


def _turns(i, refs):
    ca, sa = refs[0][pl.ds(i, 1), :], refs[1][pl.ds(i, 1), :]
    cb, sb = refs[2][:], refs[3][:]
    return ca * cb - sa * sb, sa * cb + ca * sb


def _turn(t, cos, sin):
    return (t * cos + pltpu.roll(t, HEAD // 2, 1) * sin).astype(BF)


def _turn_back(t, cos, sin):
    return (t * cos - pltpu.roll(t, HEAD // 2, 1) * sin).astype(BF)


def _rows(width, rows=ROWS):
    return pl.BlockSpec((rows, width), lambda i: (i, 0))


def _whole(a):
    return pl.BlockSpec(a.shape, lambda i: (0,) * a.ndim, pipeline_mode=ONE)


def _of_layer(w, number):
    return pl.BlockSpec((1, *w.shape[1:]), lambda i: (number, 0, 0), pipeline_mode=ONE)


def _attend(q_ref, k_s, v_s, o_ref, lse_ref, top_s, mix_s, row, group):
    bq, width = q_ref.shape
    heads = width // HEAD
    e = HEAD**-0.5 * LOG2E
    ones = jnp.ones((8, bq), BF)
    top_s[:] = jnp.full(top_s.shape, NEG, F32)
    _zero(mix_s)

    def block(j, masked):
        here = pl.ds(pl.multiple_of(j * bq, bq), bq)
        kept = _hidden(bq, bq) if masked else None
        scores = [_nt(k_s[here, _cols(n // group)], q_ref[:, _cols(n)]) for n in range(heads)]
        weights, keeps = [], []
        for n, s in enumerate(scores):
            if masked:
                s = jnp.where(kept, s, 2 * NEG)
            old = top_s[n : n + 1, :]
            top = jnp.maximum(old, s.max(axis=0, keepdims=True))
            top_s[n : n + 1, :] = top
            weights.append(jnp.exp2((s - top) * e).astype(BF))
            keeps.append(jnp.exp2((old - top) * e))
        values = [jnp.concatenate([v_s[here, _cols(g)].T, ones], axis=0) for g in range(heads // group)]
        for n, (p, keep) in enumerate(zip(weights, keeps)):
            mix_s[n] = mix_s[n] * keep + _nn(values[n // group], p)

    _loop(row, lambda j: block(j, False))
    block(row, True)
    for n in range(heads):
        total = mix_s[n, HEAD : HEAD + 1, :]
        o_ref[:, _cols(n)] = (mix_s[n, :HEAD, :] * (1 / total)).T.astype(BF)
        lse_ref[n : n + 1, :] = top_s[n : n + 1, :] * e + jnp.log2(total)


def _hidden(*shape):
    return lax.broadcasted_iota(jnp.int32, shape, 1) >= lax.broadcasted_iota(jnp.int32, shape, 0)


def _forward_kernel(x_ref, wq_ref, wk_ref, wv_ref, ca, sa, cb, sb, *refs, layers, blocks, group):
    take = iter(refs)
    some = lambda n: [next(take) for _ in range(n)]
    hbm = some(4)
    q_ref, k_ref, v_ref, o_ref, lse_ref, mid_ref, out_ref, bt_ref, *kept_hbm = some(10)
    k_s, v_s, h_s, top_s, mix_s, p_s, kept_s, load, sem, *weights = some(13)
    i = pl.program_id(0)
    row, layer = lax.rem(i, blocks), lax.div(i, blocks)
    here = _rows_at(row)
    loads = [pltpu.make_async_copy(ref.at[0], buf, load.at[n]) for n, (ref, buf) in enumerate(zip(hbm, weights))]
    tiles = kept_s.shape[1]

    def keeps(row):
        return [pltpu.make_async_copy(kept_s.at[w, n], ref.at[n, _rows_at(row), :], sem.at[w, n]) for n in range(tiles) for w, ref in enumerate(kept_hbm)]

    @pl.when(i == 0)
    def _():
        _run(loads)
        h_s[:] = jnp.zeros(h_s.shape, BF)

    cos, sin = _turns(row, (ca, sa, cb, sb))
    h = jnp.where(layer == 0, x_ref[:], h_s[here, :])
    a = _norm(h)[0].astype(BF)
    for w_ref, out in ((wq_ref, q_ref), (wk_ref, k_ref)):
        for at in range(w_ref.shape[2] // THIRD):
            t = _nn(a, w_ref[0, :, _cols(at, THIRD)]).astype(BF).astype(F32)
            for n in range(THIRD // HEAD):
                out[:, _cols(at * 2 + n)] = _turn(t[:, _cols(n)], cos, sin)
    v = _nn(a, wv_ref[0]).astype(BF)
    v_ref[:] = v
    v_s[here, :] = v
    k_s[here, :] = k_ref[:]
    _attend(q_ref, k_s, v_s, o_ref, lse_ref, top_s, mix_s, row, group)

    @pl.when(layer < layers - 1)
    def _():
        pl.when(i == 0)(lambda: _settle(loads))
        pl.when(i > 0)(lambda: _settle(keeps(row)))
        wo, wg, wu, wd = weights
        mid = jnp.where(layer == 0, x_ref[:], h_s[here, :]) + _nn(o_ref[:], wo[:]).astype(BF)
        mid_ref[:] = mid
        b = _norm(mid)[0].astype(BF)
        bt_ref[:] = b.T
        for n in range(tiles):
            gate, up = _nn(b, wg[:, _cols(n, THIRD)]), _nn(b, wu[:, _cols(n, THIRD)])
            kept_s[0, n] = gate
            kept_s[1, n] = up
            p_s[:, _cols(n, THIRD)] = (gate * jax.nn.sigmoid(gate) * up).astype(BF)
        _run(keeps(row))
        out = mid + _nn(p_s[:], wd[:]).astype(BF)
        out_ref[:] = out
        h_s[here, :] = out

    @pl.when(i == layers * blocks - 1)
    def _():
        _settle(keeps(row))


def _rows_at(row):
    return _ds(row * ROWS, ROWS)


def forward(x, weights):
    wq, wk, wv, *feed = weights
    layers, d, ff = feed[1].shape
    s = x.shape[0]
    blocks = s // ROWS
    tables = _tables(s, ROWS)
    nq, nk = wq.shape[2], wk.shape[2]
    row = lambda width: pl.BlockSpec((ROWS, width), lambda i: (i, 0))
    first = lambda i: jnp.minimum(i, blocks - 1)
    kept = pl.BlockSpec((ROWS, d), lambda i: (first(i), 0))
    of_layer = lambda w: pl.BlockSpec((1, *w.shape[1:]), lambda i: (lax.div(i, blocks), 0, 0))
    heads = nq // HEAD
    tile = _f32(ff // THIRD, s, THIRD)
    return pl.pallas_call(
        functools.partial(_forward_kernel, layers=layers, blocks=blocks, group=heads // (nk // HEAD)),
        grid=(layers * blocks,),
        in_specs=[kept, *(of_layer(w) for w in (wq, wk, wv)), *(_whole(t) for pair in tables for t in pair), *[ANY] * 4],
        out_specs=[row(nq), row(nk), row(nk), row(nq), pl.BlockSpec((8, ROWS), lambda i: (0, i)), kept, kept, pl.BlockSpec((d, ROWS), lambda i: (0, first(i))), ANY, ANY],
        out_shape=[*(_bf(layers * s, n) for n in (nq, nk, nk, nq)), _f32(8, layers * s), _bf(s, d), _bf(s, d), _bf(d, s), tile, tile],
        scratch_shapes=[*(pltpu.VMEM(shape, BF) for shape in ((s, nk), (s, nk), (s, d))), pltpu.VMEM((8, ROWS), F32), pltpu.VMEM((heads, HEAD + 8, ROWS), F32),
                        pltpu.VMEM((ROWS, ff), BF), pltpu.VMEM((2, ff // THIRD, ROWS, THIRD), F32), DMA((4,)), DMA((2, ff // THIRD)),
                        *(pltpu.VMEM(w.shape[1:], BF) for w in feed)],
        compiler_params=_params(),
        name="forward",
    )(x, wq, wk, wv, *(t for pair in tables for t in pair), *feed)


AXES = ((8, 4, 2), (4, 2, 8), (2, 8, 4))
CORE = 1
HALF = THIRD // 2
QUARTER = HALF // 2
EIGHTH = QUARTER // 2
NEAR = (CORE, *AXES[0])
MESH = pl.DeviceIdType.MESH
SIDES = 4


def _bit(stride):
    return lax.rem(lax.div(lax.axis_index("dp"), stride), 2)


def _peer(stride):
    return {"dp": lax.axis_index("dp") + stride * (1 - 2 * _bit(stride))}


def _greet(peers):
    barrier = pltpu.get_barrier_semaphore()
    for peer in peers:
        pl.semaphore_signal(barrier, device_id=peer, device_id_type=MESH)
    pl.semaphore_wait(barrier, len(peers))


def _send(src, dst, sems, at, peer):
    return pltpu.make_async_remote_copy(src, dst, sems[0].at[at], sems[1].at[at], device_id=peer, device_id_type=MESH)


class Scatter:
    def __init__(self, mine, dst, bufs, sems):
        self.mine, self.dst, self.sems = mine, dst, sems
        self.r0, *self.got, self.sum = bufs

    @staticmethod
    def scratch(width, slots):
        rows = (HALF, QUARTER, EIGHTH, PART, HALF)
        return [pltpu.VMEM((slots, 3, n, width), BF) for n in (THIRD, *rows)] + [DMA((slots, 3, 5))] * 2

    @staticmethod
    def of(scratch, n, dst):
        mine, *bufs, sent, got = [ref.at[lax.rem(n, ref.shape[0])] for ref in scratch]
        return Scatter(mine, dst, bufs, (sent, got))

    def _core(self, t, late):
        b = _bit(AXES[t][0])
        at = QUARTER * (b if late else 1 - b)
        return _send(self.mine.at[t, _ds(HALF * (1 - _bit(CORE)) + at, QUARTER), :], self.r0.at[t, _ds(at, QUARTER), :], self.sems, (t, 3 + late), _peer(CORE))

    def _over(self, t, k):
        size = QUARTER >> k
        return _send(self.sum.at[t, HALF - 2 * size : HALF - size, :], self.got[k].at[t], self.sems, (t, k), _peer(AXES[t][k]))

    def start(self):
        for late in (False, True):
            for t in THIRDS:
                self._core(t, late).start()

    def _add(self, t, k, dst):
        bits = [_bit(stride) for stride in AXES[t]]
        if k < 3:
            bits[k] = 1 - bits[k]
        size = QUARTER >> min(k, 2)
        at = [sum(b * (QUARTER >> n) for n, b in list(enumerate(bits[: k + 1]))[m:]) for m in range(min(k, 2) + 2)]
        total = self.mine[t, _ds(HALF * _bit(CORE) + at[0], size), :].astype(F32) + self.r0[t, _ds(at[0], size), :].astype(F32)
        for n in range(k):
            total += self.got[n][t, _ds(at[n + 1] if n < 2 else 0, size), :].astype(F32)
        dst[:] = total.astype(BF)

    def halve(self, k):
        for t in THIRDS:
            if k < 2:
                self._core(t, bool(k)).wait()
            if k:
                self._over(t, k - 1).wait()
        size = QUARTER >> k
        for t in THIRDS:
            self._add(t, k, self.sum.at[t, HALF - 2 * size : HALF - size, :])
        for t in THIRDS:
            self._over(t, k).start()

    def finish(self):
        for t in THIRDS:
            self._over(t, 2).wait()
        for t in THIRDS:
            self._add(t, 3, self.dst.at[t])


class Gather:
    def __init__(self, own, everything, sems):
        self.own, self.all, self.sems = own, everything, sems

    @staticmethod
    def scratch(own):
        return [pltpu.VMEM(own.shape, BF), DMA((4,)), DMA((3, 9)), DMA((3, 9))]

    def _move(self, t, k, axis=True):
        bits = [_bit(CORE), *(_bit(stride) for stride in AXES[t])]
        over = THIRDS[-1 - min(max(k, 0), 2)]
        if k == 3:
            bits[2] = 1 - bits[2]
        if k >= 0 and not axis:
            bits[1 + over] = 1 - bits[1 + over]
        count = 1 << min(max(k, 0), 1)
        there = self.all.at[t, pl.ds(sum(b * (8 >> n) for n, b in enumerate(bits) if 8 >> n >= count), count)]
        src = there if k > 0 or not axis and k == 0 else self.own.at[pl.ds(t, 1)]
        return _send(src, there, self.sems, (t, k if axis else 5 + k), _peer(AXES[t][over] if axis else CORE))

    def place(self, sem):
        return [pltpu.make_async_copy(self.own.at[pl.ds(t, 1)], self._move(t, -1, False).dst_ref, sem.at[t]) for t in THIRDS]

    def start(self):
        for t in THIRDS:
            self._move(t, 0).start()
            self._move(t, -1, False).start()

    def double(self, k):
        for t in THIRDS:
            self._move(t, k).wait_recv()
            if k == 0:
                self._move(t, 1).start()
            elif k == 1:
                self._move(t, 3).start()
            self._move(t, k, False).start()
        if k == 0:
            for t in THIRDS:
                self._move(t, 2).start()

    def finish(self):
        for t in THIRDS:
            for k in range(4):
                self._move(t, k).wait_send()
                self._move(t, k, False).wait()
            self._move(t, -1, False).wait()


class Gathers:
    def __init__(self, own, everything, scratch):
        self.units = []
        for n, (o, a) in enumerate(zip(own, everything)):
            stage, sem, *sems = scratch[4 * n : 4 * n + 4]
            self.units.append((Gather(stage, a, sems), pltpu.make_async_copy(o, stage, sem.at[3]), sem))

    def load(self):
        _run([load for _, load, _ in self.units])

    def start(self):
        for g, load, sem in self.units:
            load.wait()
            g.start()
            _run(g.place(sem))

    def double(self, k):
        for g, _, sem in self.units:
            if k == 0:
                _settle(g.place(sem))
            g.double(k)

    def finish(self):
        for g, *_ in self.units:
            g.finish()

    @staticmethod
    def outs(parts):
        return [_bf(3, PART, *p.shape[1:]) for p in parts]

    @staticmethod
    def scratch(parts):
        return [s for p in parts for s in Gather.scratch(p)]


def _feed_back_kernel(*refs, fresh, number, tiles, guest):
    take = iter(refs)
    some = lambda n: [next(take) for _ in range(n)]
    o_hbm, mid_hbm, dy_hbm, wo_hbm, wg_hbm, wu_hbm, wd_hbm = some(7)
    kept = [] if fresh else some(3)
    guests = some(min(guest, 1))
    by_hbm, do_hbm, delta_ref, own_ref = some(4)
    guest_all = some(min(guest, 1))
    dy_s, wo_s, wg_s, wu_s, dg_s, du_s, load, pair_sem = some(8)
    room = some(8)
    gathers = [(Gather(own_ref.at[:, :guest], ref, some(2)), some(1)[0]) for ref in guest_all]
    tile_s = room[0]
    slots = tile_s.shape[0]
    s, d = dy_s.shape
    width = THIRD
    blocks = s // ROWS
    rows = _rows_at
    halves = [functools.partial(Scatter.halve, k=k) for k in THIRDS]

    run, settle = _run, _settle

    def tell(now, acts):
        for act, back, first, last in acts:
            n = now - back

            @pl.when((n >= first) & (n <= last))
            def _():
                act(Scatter.of(room, n + 2 * guest, own_ref.at[:, n + guest]))

    def acts(last):
        backs = (Scatter.finish, slots), (halves[2], slots - 1), (halves[1], slots - 2), (halves[0], 2), (Scatter.start, 1)
        return [(act, back, -guest, last if back > 2 else tiles - 1) for act, back in backs]

    def row_loads(r, bufs):
        here = rows(r) if fresh else slice(None)
        there = _rows_at(number * blocks + r), rows(r)
        return [pltpu.make_async_copy(hbm.at[at, :], buf.at[here, :], pair_sem.at[n]) for n, (hbm, at, buf) in enumerate(zip((o_hbm, mid_hbm), there, bufs))]

    late_loads = [pltpu.make_async_copy(hbm.at[number], buf, load.at[n]) for n, (hbm, buf) in enumerate(((wo_hbm, wo_s), (wg_hbm, wg_s), (wu_hbm, wu_s)))]

    def tile_phase(wd_s, wd_sem, bt_s, p_s, *more):
        pairs = [(dy_hbm, dy_s)] if fresh else [(dy_hbm, dy_s), (kept[2], bt_s.at[:, :s])]
        pairs += [(ref.at[n], tile_s.at[(n + guest) % slots]) for ref in guests for n in range(guest)]
        loads = [pltpu.make_async_copy(*pair, load.at[3 + n]) for n, pair in enumerate(pairs)]

        def down(n):
            slot = lax.rem(n, 2)
            return pltpu.make_async_copy(wd_hbm.at[number, _ds(lax.rem(n, tiles) * width, width), :], wd_s.at[slot], wd_sem.at[slot])

        def fetch(n):
            slot = lax.rem(n, 2)
            return [pltpu.make_async_copy(ref.at[lax.rem(n, tiles)], more[0].at[slot, w], more[1].at[slot, w]) for w, ref in enumerate(kept[:2])]

        run([down(0)] + (row_loads(0, more[1:]) + late_loads + loads if fresh else loads[::-1] + fetch(0)))
        _greet([_peer(stride) for stride in NEAR])
        settle(loads[2:])
        _loop(max(guest - 1, 0), lambda n: tell(n + 1 - guest, acts(0)))
        if fresh:
            b_s, *bufs = more
            o_s, mid_s = bufs
            settle(late_loads[:1])

            def prepare(r):
                settle(row_loads(r, bufs))
                pl.when(r + 1 < blocks)(lambda: run(row_loads(r + 1, bufs)))
                mid = mid_s[rows(r), :] + _nn(o_s[rows(r), :], wo_s[:]).astype(BF)
                mid_s[rows(r), :] = mid
                b = _norm(mid)[0].astype(BF)
                b_s[rows(r), :] = b
                bt_s[:, _ds(r * ROWS, ROWS, ROWS)] = b.T

            _loop(blocks, prepare)
            settle(late_loads[1:] + loads)
        else:
            settle(loads[:2])
            run(late_loads)

        def tile(i):
            tell(i, acts(tiles))
            pl.when(i == tiles - 1)(begin)
            f = _ds(i * width, width, width)
            settle([down(i)] + fetch(i))
            run([down(i + 1)] + fetch(i + 1))
            wd = wd_s[lax.rem(i, 2)]
            for r in range(blocks):
                here = _cols(r, ROWS)
                if fresh:
                    gate, up = _nn(b_s[here, :], wg_s[:, f]), _nn(b_s[here, :], wu_s[:, f])
                else:
                    gate, up = (more[0][lax.rem(i, 2), w, here, :] for w in range(2))
                dp = _nt(dy_s[here, :], wd).astype(BF).astype(F32)
                sig = jax.nn.sigmoid(gate)
                silu = gate * sig
                p_s[here, :] = (silu * up).astype(BF)
                du_s[here, f] = (dp * silu).astype(BF)
                dg_s[here, f] = (dp * up * (sig * (1 + gate * (1 - sig)))).astype(BF)
            new = tile_s.at[lax.rem(i + 2 * guest, slots)]
            for n, right in enumerate((dg_s[:, f], du_s[:, f])):
                out = _nn(bt_s[:, :s], right).astype(BF)
                for t in THIRDS:
                    new[t, :, _cols(n, width)] = out[_cols(t, THIRD), :]
            out = _tn(p_s[:], dy_s[:]).astype(BF)
            for t in THIRDS:
                new[t, :, 2 * width :] = out[:, _cols(t, width)]

        _loop(tiles, tile)
        settle([down(tiles)] + fetch(tiles))

    def begin():
        for gather, sem in gathers:
            gather.start()
            _run(gather.place(sem))

    def row_phase(by_s, do_s, sem, *bufs):
        def row_stores(r):
            return [pltpu.make_async_copy(buf, hbm.at[rows(r), :], sem.at[n]) for n, (hbm, buf) in enumerate(((by_hbm, by_s), (do_hbm, do_s)))]

        if not fresh:
            settle(late_loads)

        def row(r):
            tell(tiles + r, acts(tiles - 2) + [(halves[1 + n], slots - 3 + n, tiles - 1, tiles - 1) for n in (1, 0)])
            for gather, sem in gathers:
                pl.when(r == 0)(lambda: _settle(gather.place(sem)))
                for k in range(blocks):
                    pl.when(r == k)(functools.partial(gather.double, k))
            here = rows(r)
            part = here if fresh else slice(None)
            if not fresh:
                run(row_loads(r, bufs))
            db = (_nt(dg_s[here, :], wg_s[:]) + _nt(du_s[here, :], wu_s[:])).astype(BF).astype(F32)
            if not fresh:
                settle(row_loads(r, bufs))
            pl.when(r > 0)(lambda: settle(row_stores(r - 1)))
            o_s, mid_s = bufs
            xhat, scale = _norm(mid_s[part, :])
            by = dy_s[here, :] + _norm_back(xhat, scale, db).astype(BF)
            by_s[:] = by
            do = _nt(by, wo_s[:]).astype(BF)
            do_s[:] = do
            run(row_stores(r))
            both = do.astype(F32) * o_s[part, :].astype(F32)
            for n in range(d // HEAD):
                delta_ref[n : n + 1, _ds(r * ROWS, ROWS, ROWS)] = both[:, _cols(n)].T.sum(axis=0, keepdims=True)

        _loop(blocks, row)
        settle(row_stores(blocks - 1))

    vmem = lambda *shape: pltpu.VMEM(shape, BF)
    kinds = [vmem(2, width, d), DMA((2,)), vmem(d, s + HEAD), vmem(s, width)]
    out = [vmem(ROWS, d), vmem(ROWS, d)]
    if fresh:

        def all_phases(*bufs):
            pl.run_scoped(lambda *a: tile_phase(*a, *bufs), *kinds, vmem(s, d))
            pl.run_scoped(lambda *a: row_phase(*a, *bufs), *out, DMA((2,)))

        pl.run_scoped(all_phases, vmem(s, d), vmem(s, d))
    else:
        pl.run_scoped(tile_phase, *kinds, pltpu.VMEM((2, 2, s, width), F32), DMA((2, 2)))
        pl.run_scoped(row_phase, *out, DMA((2,)), *out)
    for n in (tiles - 2, tiles - 1):
        Scatter.of(room, n + 2 * guest, own_ref.at[:, n + guest]).finish()
    for gather, _ in gathers:
        gather.finish()


def feed_back(o, h, dy, weights, number, collective_id, kept=(), guest=(), slots=6):
    s, d = h.shape
    ff = weights[1].shape[2]
    tiles = ff // THIRD
    fresh = not kept
    tiles_in = guest[0].shape[0] if guest else 0
    own = _bf(3, tiles_in + tiles, PART, d)
    scratch = [pltpu.VMEM(shape, BF) for shape in ((s, d), *(w.shape[1:] for w in weights[:3]), (s, ff), (s, ff))]
    in_vmem = pl.BlockSpec(memory_space=pltpu.VMEM)
    return pl.pallas_call(
        functools.partial(_feed_back_kernel, fresh=fresh, number=number, tiles=tiles, guest=tiles_in),
        in_specs=[ANY] * (7 + len(kept) + len(guest)),
        out_specs=[ANY, ANY, in_vmem, in_vmem, *[ANY] * len(guest)],
        out_shape=[_bf(s, d), _bf(s, d), _f32(8, s), own, *(_bf(3, PART, tiles_in, PART, d) for _ in guest)],
        scratch_shapes=[*scratch, DMA((8,)), DMA((2,)), *Scatter.scratch(d, slots), *[DMA((3, 9)), DMA((3, 9)), DMA((3,))] * len(guest)],
        compiler_params=_params(collective_id=collective_id, has_side_effects=True),
        name="feed_back",
    )(o, h, dy, *weights, *kept, *guest)


def _attend_back_kernel(q_ref, k_ref, v_ref, do_ref, lse_ref, delta_ref, *rest, bk, group, units, first):
    own, rest = rest[:units], rest[units:]
    dq_ref, dk_ref, dv_ref, *rest = rest
    everything, rest = rest[:units], rest[units:]
    dq_s, dk_s, dv_s, *rest = rest
    work = Gathers([ref.at[:, first:] for ref in own], everything, rest)
    bq, width = q_ref.shape
    heads = width // HEAD
    iq = pl.program_id(0)
    last = pl.num_programs(0) - 1
    scale = HEAD**-0.5
    e = scale * LOG2E

    @pl.when(iq == 0)
    def _():
        work.load()
        _greet([_peer(stride) for stride in NEAR])
        work.start()
        _zero(dk_s, dv_s)

    _zero(dq_s)

    def block(j, first):
        here = _ds(j * bk, bk)
        at = first or 0
        kept = None if first is None else _hidden(bk, bq - at)
        scores, dps = [], []
        for n in range(heads):
            g = n // group
            scores.append(_nt(k_ref[here, _cols(g)], q_ref[at:, _cols(n)]))
            dps.append(_nt(v_ref[here, _cols(g)], do_ref[at:, _cols(n)]))
        for n in range(heads):
            g = n // group
            p = jnp.exp2(scores[n] * e - lse_ref[n : n + 1, at:])
            if first is not None:
                p = jnp.where(kept, p, 0.0)
            ds = (p * (dps[n] - delta_ref[n : n + 1, at:])).astype(BF)
            dv_s[g, here, :] += _nn(p.astype(BF), do_ref[at:, _cols(n)])
            dk_s[g, here, :] += _nn(ds, q_ref[at:, _cols(n)])
            dq_s[n, :, at:] += _nn(k_ref[here, _cols(g)].T, ds)

    per = bq // bk
    _loop(iq * per, lambda j: block(j, None))
    for n in THIRDS:
        pl.when(iq == last - 2 + n)(functools.partial(work.double, n))
    for n in range(per):
        block(iq * per + n, n * bk)
    pl.when(iq == last)(lambda: work.double(3))
    for n in range(heads):
        dq_ref[:, _cols(n)] = (dq_s[n] * scale).T.astype(BF)

    @pl.when(iq == last)
    def _():
        for g in range(heads // group):
            dk_ref[:, _cols(g)] = (dk_s[g] * scale).astype(BF)
            dv_ref[:, _cols(g)] = dv_s[g].astype(BF)
        work.finish()


def attend_back(q, k, v, do, lse, delta, parts, first, number, collective_id, bq=ROWS, bk=THIRD):
    s, width = do.shape
    heads, groups = width // HEAD, k.shape[1] // HEAD
    base = number * (s // bq)
    mine = lambda a: pl.BlockSpec((s, a.shape[1]), lambda i: (number, 0), pipeline_mode=ONE)
    out = [_bf(s, t.shape[1]) for t in (q, k, v)]
    mine_own = [_bf(3, p.shape[1] - first, *p.shape[2:]) for p in parts]
    return pl.pallas_call(
        functools.partial(_attend_back_kernel, bk=bk, group=heads // groups, units=len(parts), first=first),
        grid=(s // bq,),
        in_specs=[pl.BlockSpec((bq, width), lambda i: (base + i, 0)), mine(k), mine(v), _rows(width, bq), pl.BlockSpec((8, bq), lambda i: (0, base + i)),
                  pl.BlockSpec((8, bq), lambda i: (0, i)), *[ANY] * len(mine_own)],
        out_specs=[_rows(width, bq), *(_whole(t) for t in out[1:]), *[ANY] * len(mine_own)],
        out_shape=[*out, *Gathers.outs(mine_own)],
        scratch_shapes=[pltpu.VMEM(shape, F32) for shape in ((heads, HEAD, bq), (groups, s, HEAD), (groups, s, HEAD))] + Gathers.scratch(mine_own),
        compiler_params=_params(collective_id=collective_id, has_side_effects=True),
        name="attend_back",
    )(q, k, v, do, lse, delta, *parts)


def _squares(ref, total):
    tiles = ref.shape[1]

    def one(n, total):
        g = ref[lax.div(n, tiles), lax.rem(n, tiles)].astype(F32)
        return total + g * g

    return lax.fori_loop(0, len(THIRDS) * tiles, one, total)


Q, KV, OUT = THIRDS


def _proj_back_kernel(*refs, parts, devices, number):
    take = iter(refs)
    some = lambda n: [next(take) for _ in range(n)]
    h_hbm, by_hbm, o_hbm, dq_hbm, dk_hbm, dv_hbm, *tables = some(10)
    deep = parts == 0
    if deep:
        w_hbm = some(3)
        out_hbm, g_hbm = some(2)
    else:
        parts = some(parts)
        size_ref, all_ref = some(2)
    h_s, by_s, o_s, t_s, at_s, load, tile_s = some(7)
    s, d = h_s.shape
    nq, nk = dq_hbm.shape[1], dk_hbm.shape[1]
    blocks = s // ROWS
    spots = [slice(0, nq), slice(nq, nq + nk), slice(nq + nk, nq + 2 * nk)]
    pairs = [(o_hbm.at[_ds(number * s, s), :], o_s), (by_hbm, by_s), (h_hbm, h_s), *((ref, t_s.at[:, at]) for ref, at in zip((dq_hbm, dk_hbm, dv_hbm), spots))]
    loads = [pltpu.make_async_copy(*pair, load.at[n]) for n, pair in enumerate(pairs)]
    _run(loads)
    if deep:
        w_s, out_s, sems = some(3)
        weights = [pltpu.make_async_copy(ref.at[number], w_s.at[:, at], sems.at[n]) for n, (ref, at) in enumerate(zip(w_hbm, spots))]
        _run(weights)
    else:
        room = [tile_s, *some(7)]
        own_s, local, slots, *sems = some(9)
        tiles = own_s.shape[1]
        work = [Scatter.of(room, n, own_s.at[:, n]) for n in range(tiles)]
        gathers = [Gather(own_s.at[:, at], all_ref.at[:, :, at], pair) for at, pair in ((slice(OUT), sems[:OUT]), (slice(OUT, tiles), sems[OUT:SIDES]))]
        places = [g.place(local.at[n]) for n, g in enumerate(gathers)]
        me = lax.axis_index("dp")
        others = [lax.rem(me + n, devices) for n in range(1, devices)]
        _greet([{"dp": other} for other in others])

    def put(n, value):
        for t in THIRDS:
            tile_s[n, t, :, : value.shape[1]] = value[_cols(t, THIRD), :].astype(BF)

    def prepare(r):
        here = _rows_at(r)
        cos, sin = _turns(r, tables)
        for n in range((nq + nk) // HEAD):
            t_s[here, _cols(n)] = _turn_back(t_s[here, _cols(n)].astype(F32), cos, sin)
        xhat, scale = _norm(h_s[here, :])
        at_s[:, _ds(r * ROWS, ROWS, ROWS)] = xhat.astype(BF).T
        return xhat, scale

    def store(r):
        return pltpu.make_async_copy(out_s.at[lax.rem(r, 2)], out_hbm.at[_rows_at(r), :], sems.at[lax.rem(r, 2)])

    def row(r):
        xhat, scale = prepare(r)
        here = _rows_at(r)
        da = _nt(t_s[here, :], w_s[:]).astype(BF).astype(F32)
        pl.when(r > 1)(lambda: store(r - 2).wait())
        out_s[lax.rem(r, 2)] = by_s[here, :] + _norm_back(xhat, scale, da).astype(BF)
        store(r).start()

    _settle(loads[:OUT])
    put(OUT, _tn(o_s[:], by_s[:]))
    if not deep:
        work[OUT].start()
    _settle(loads[OUT:])
    if deep:
        _settle(weights)
        _loop(blocks, row)
    else:
        _loop(blocks, lambda r: prepare(r) and None)
        work[OUT].halve(Q)
    put(Q, _nn(at_s[:, :s], t_s[:, :nq]))
    if not deep:
        work[Q].start()
        work[OUT].halve(KV)
    put(KV, jnp.zeros((d, d), BF))
    put(KV, _nn(at_s[:, :s], t_s[:, nq:]))
    if deep:
        g_copy = pltpu.make_async_copy(tile_s, g_hbm, load.at[0])
        g_copy.start()
        _settle([store(blocks - 2), store(blocks - 1), g_copy])
        return
    work[KV].start()
    work[OUT].halve(OUT)
    work[Q].halve(Q)
    total = jnp.zeros((PART, d), F32)
    for ref in parts:
        total = _squares(ref, total)
    work[KV].halve(Q)
    work[OUT].finish()

    def begin(n):
        gathers[n].start()
        _run(places[n])

    def double(n, k):
        if k == Q:
            _settle(places[n])
        gathers[n].double(k)

    begin(KV)
    for k in (KV, OUT):
        for n in (Q, KV):
            work[n].halve(k)
    double(KV, Q)
    for n in (Q, KV):
        work[n].finish()
    begin(Q)
    slots[me] = jnp.full(size_ref.shape, jnp.sum(_squares(own_s, total)), F32)
    copies = [_send(slots.at[me], slots.at[me], sems[SIDES:], n, {"dp": other}) for n, other in enumerate(others)]
    _run(copies)
    double(KV, KV)
    double(Q, Q)
    double(KV, OUT)
    _settle(copies)
    size_ref[:] = sum(slots[n] for n in range(devices))
    double(KV, len(THIRDS))
    for k in range(KV, SIDES):
        double(Q, k)
    for g in gathers:
        g.finish()


def proj_back(h, by, o, dq, dk, dv, weights=(), number=0, parts=(), devices=0, collective_id=0):
    s, d = h.shape
    (ca, sa), (cb, sb) = _tables(s, ROWS)
    wide = dq.shape[1] + 2 * dk.shape[1]
    vmem = lambda *shape: pltpu.VMEM(shape, BF)
    in_vmem = pl.BlockSpec(memory_space=pltpu.VMEM)
    scratch = [*[vmem(s, d)] * 3, vmem(s, wide), vmem(d, s + HEAD), DMA((6,))]
    own = _bf(3, 3, PART, d)
    if weights:
        scratch += [vmem(3, 3, THIRD, d), vmem(d, wide), vmem(2, ROWS, d), DMA((3,))]
        outs = [ANY] * 2, [_bf(s, d), _bf(3, 3, THIRD, d)]
    else:
        scratch += Scatter.scratch(d, 3) + [vmem(*own.shape), DMA((2, 3)), pltpu.VMEM((devices, 8, HEAD), F32), *[DMA((3, 9))] * SIDES, *[DMA((devices,))] * 2]
        outs = [in_vmem, ANY], [_f32(8, HEAD), *Gathers.outs([own])]
    return pl.pallas_call(
        functools.partial(_proj_back_kernel, parts=len(parts), devices=devices, number=number),
        in_specs=[*[ANY] * 6, *[in_vmem] * 4, *[ANY] * len(weights), *[in_vmem] * len(parts)],
        out_specs=outs[0],
        out_shape=outs[1],
        scratch_shapes=scratch,
        compiler_params=_params() if weights else _params(collective_id=collective_id, has_side_effects=True),
        name="proj_back",
    )(h, by, o, dq, dk, dv, ca, sa, cb, sb, *weights, *parts)


KINDS = (BF, F32, F32) * 2
NEW = range(3, len(KINDS))


def _update_kernel(size_ref, *refs, layers, slots, count):
    take = iter(refs)
    some = lambda n: [next(take) for _ in range(n)]
    proj, feed = some(layers), some(layers)
    hbm = [some(len(NAMES)) for _ in KINDS]
    flat, deep = some(len(KINDS)), some(len(KINDS))
    gp_s, gf_s, in_sem, g_sem, out_sem = take
    rows = flat[0].shape[1]
    sixteenths = rows // PART
    tiles = gf_s.shape[2]
    steps = 3 * PART // sixteenths
    factor = jnp.minimum(1.0, 0.5 * lax.rsqrt(size_ref[0:1, 0:1] / count + 1e-30))
    narrow = flat[0].shape[2] - 2 * tiles * THIRD

    def moves(k, layer, i, slot):
        sem = out_sem.at[slot, k % 3] if k in NEW else in_sem.at[slot, k]
        at = 0
        for ref in hbm[k][:6]:
            there, here = ref.at[layer, _ds(i * rows, rows), :], flat[k].at[slot, :, at : at + ref.shape[2]]
            yield pltpu.make_async_copy(here, there, sem) if k in NEW else pltpu.make_async_copy(there, here, sem)
            at += ref.shape[2]
        per = PART // sixteenths
        there = hbm[k][6].at[layer, :, _ds(lax.rem(i, per) * rows, rows), _ds(lax.div(i, per) * THIRD, THIRD, THIRD)]
        yield pltpu.make_async_copy(deep[k].at[slot], there, sem) if k in NEW else pltpu.make_async_copy(there, deep[k].at[slot], sem)

    def fetch(layer, i, slot):
        per = PART // sixteenths
        for n, (ref, buf) in enumerate(((proj[layer], gp_s), (feed[layer], gf_s))):
            pltpu.make_async_copy(ref.at[lax.div(i, per), pl.ds(lax.rem(i, per) * sixteenths, sixteenths)], buf.at[slot], g_sem.at[slot, n]).start()
        for k in THIRDS:
            for c in moves(k, layer, i, slot):
                c.start()

    def settled(k, slot):
        sem = out_sem.at[slot, k % 3] if k in NEW else in_sem.at[slot, k]
        for buf in (flat[k], deep[k]):
            pltpu.make_async_copy(buf.at[slot], buf.at[slot], sem).wait()

    def advance(g, bufs, at):
        g = g.astype(F32) * factor
        w, m, v = (buf[at].astype(F32) for buf in bufs[:3])
        m = 0.9 * m + 0.1 * g
        v = 0.95 * v + 0.05 * g * g
        for buf, new in zip(bufs[3:], (w - 0.02 * (m * lax.rsqrt(v + 1e-8) + 0.1 * w), m, v)):
            buf[at] = new.astype(buf.dtype)

    def one(layer):
        def step(i):
            n = layer * steps + i
            slot = lax.rem(n, slots)

            @pl.when(n >= slots)
            def _():
                for k in NEW:
                    settled(k, slot)

            for n, buf in enumerate((gp_s, gf_s)):
                pltpu.make_async_copy(buf.at[slot], buf.at[slot], g_sem.at[slot, n]).wait()
            for k in THIRDS:
                settled(k, slot)

            def tile(f):
                for n in range(sixteenths):
                    here = _cols(n, PART)
                    for w in range(2):
                        advance(gf_s[slot, n, f, :, _cols(w, THIRD)], flat, (slot, here, _ds(narrow + (w * tiles + f) * THIRD, THIRD, THIRD)))
                    advance(gf_s[slot, n, f, :, 2 * THIRD :], deep, (slot, f, here))

            _loop(tiles, tile)

            def plain(f):
                for n in range(sixteenths):
                    across = _ds(f * THIRD, THIRD, THIRD)
                    place = jnp.where(f < 5, f, f + 1)
                    g = gp_s[slot, n, lax.div(place, 3), :, _ds(lax.rem(place, 3) * THIRD, THIRD, THIRD)]
                    advance(g, flat, (slot, _cols(n, PART), across))

            _loop(narrow // THIRD, plain)
            for k in NEW:
                for c in moves(k, layer, i, slot):
                    c.start()
            ahead = i + slots
            pl.when(ahead < steps)(lambda: fetch(layer, ahead, slot))
            if layer + 1 < layers:
                pl.when(ahead >= steps)(lambda: fetch(layer + 1, ahead - steps, slot))

        _loop(steps, step)

    for slot in range(slots):
        fetch(0, slot, slot)
    for layer in range(layers):
        one(layer)
    for slot in range(slots):
        for k in NEW:
            settled(k, slot)


def update(size, proj, feed, weights, m, v, slots=3, sixteenths=2):
    layers, d, ff = weights[4].shape
    rows = sixteenths * PART
    split = lambda a: a.reshape(layers, -1, THIRD, d)
    state = [a for kind in (weights, m, v) for a in (*kind[:6], split(kind[6]))]
    flat = [pltpu.VMEM((slots, rows, sum(w.shape[2] for w in weights[:6])), kind) for kind in KINDS]
    deep = [pltpu.VMEM((slots, ff // THIRD, rows, THIRD), kind) for kind in KINDS]
    grads = [pltpu.VMEM((slots, sixteenths, *g.shape[2:]), BF) for g in (proj[0], feed[0])]
    count = sum(w.size for w in weights)
    new = pl.pallas_call(
        functools.partial(_update_kernel, layers=layers, slots=slots, count=count),
        in_specs=[pl.BlockSpec(memory_space=pltpu.VMEM), *[ANY] * (2 * layers + 21)],
        out_specs=[ANY] * 21,
        out_shape=[jax.ShapeDtypeStruct(a.shape, a.dtype) for a in state],
        scratch_shapes=[*flat, *deep, *grads, DMA((slots, 3)), DMA((slots, 2)), DMA((slots, 3))],
        compiler_params=_params(),
        name="update",
    )(size, *proj, *feed, *state)
    return [a.reshape(old.shape) for a, old in zip(new, (*weights, *m, *v))]


def solution(mesh):
    devices = mesh.shape["dp"]

    def step(x, dy, *arrays):
        weights, m, v = (arrays[i : i + 7] for i in (0, 7, 14))
        wq, wk, wv, *feeds = weights
        layers = wq.shape[0]
        q, k, v_, o, lse, mid, out, *kept = forward(x[0], weights)
        by, guest = dy[0], ()
        parts, proj, feed = [], [], [None] * layers
        for n in reversed(range(layers)):
            last = n == layers - 1
            h = out if n else x[0]
            by, do, delta, own, *more = feed_back(o, h if last else mid, by, feeds, n, 2 * n + 1, () if last else (kept[1], kept[2], kept[0]), guest)
            proj += more
            dq, dk, dv, feed[n] = attend_back(q, k, v_, do, lse, delta, [own], 0 if last else wq.shape[1] // THIRD, n, 2 * n + 2)
            parts.append(own)
            if n:
                by, *guest = proj_back(h, by, o, dq, dk, dv, (wq, wk, wv), n)
        size, *first = proj_back(h, by, o, dq, dk, dv, parts=parts, devices=devices)
        return tuple(update(size, first + proj, feed, weights, m, v))

    states, all_of = P(("rep", "dp")), P()
    return jax.shard_map(
        step,
        mesh=mesh,
        in_specs=(states, states) + (all_of,) * 21,
        out_specs=(P("rep"),) * 21,
        check_vma=False,
    )
```
